256 devices in a mesh: ctx: 32 (over x, z_lo, core), tp: 8 (over z_hi, y).
Axes of the slice: x: 4, y: 4, z: 8 (z_hi: 2, z_lo: 4; z = z_hi * 4 + z_lo), core: 2. Of those that a mesh axis runs over, the one named last changes fastest.
Arguments:
- token_ids: int32 [24576], P('ctx'), may hold values from 0 to 511
- embed_table: bfloat16 [512, 4096], replicated, may hold values from -6 to 6
- norm_gain: float32 [4096], replicated, may hold values from 0.25 to 1.75
- w_in: bfloat16 [4096, 3, 2048], P(None, None, 'tp'), may hold values from -0.09375 to 0.09375
- short_taps: float32 [3, 3, 2048], P(None, None, 'tp'), may hold values from -3 to 3
- long_filter: bfloat16 [2048, 24576], P('tp', 'ctx'), may hold values from -0.0390625 to 0.0390625
- skip_gain: float32 [2048], P('tp'), may hold values from 0.5 to 2
- w_out: bfloat16 [2048, 4096], P(None, 'tp'), may hold values from -0.125 to 0.125
Outputs:
- mixed: bfloat16 [24576, 4096], P('ctx', 'tp')
The draws below stay inside these ranges and needn't reach their ends.
All inputs are finite; a program needn't handle non-finite values.
Results may differ from the reference program's by a relative error of at most 0.0095.
Values may be sent and summed in bfloat16 or wider, within the bound.
A program may use at most 128 MiB of HBM per device.

```python
import math
import jax
import jax.numpy as jnp
import numpy as np
from jax import lax

D = 4096
C = 2048
V = 512
SEQ = 24576


def touch_ends(result, stream_key, smallest, largest):
    longest = result.shape.index(max(result.shape))
    spots = []
    for shift in (0, 1):
        where = [jax.random.randint(jax.random.fold_in(stream_key, axis), (), 0, length) for axis, length in enumerate(result.shape)]
        where[longest] = (where[longest] + shift) % result.shape[longest]
        spots.append(tuple(where))
    return result.at[spots[0]].set(smallest).at[spots[1]].set(largest)


def block_levels(stream_key, extent, split, least, largest):
    def one(axis_at, parts):
        draws = jax.random.uniform(jax.random.fold_in(jax.random.fold_in(stream_key, 6), axis_at), (parts,), jnp.float32, least / len(split), largest / len(split))
        return jnp.repeat(jnp.exp(draws), extent[axis_at] // parts).reshape((-1,) + (1,) * (len(extent) - axis_at - 1))

    factor_of = one(*split[0])
    for cut in split[1:]:
        factor_of = factor_of * one(*cut)
    return factor_of


def rank_bounds(amount, lean):
    weights = [(1 << 20) // math.isqrt(grade ** lean) + 1 for grade in range(1, amount + 1)]
    deviation = 1 + sum(weights) // (1 << 30)
    return np.cumsum(np.array([max(1, weight // deviation) for weight in weights]))


def skewed_ids(rng, shape, amount, lean):
    listing = rank_bounds(amount, lean)
    ticket = jax.random.randint(jax.random.fold_in(rng, 1), shape, 0, int(listing[amount - 1]))
    grade = jnp.searchsorted(jnp.asarray(listing, jnp.int32), ticket, side="right")
    return jax.random.permutation(jax.random.fold_in(rng, 2), amount)[grade].astype(jnp.int32)


def scatter_about(rng, dims, deviation, limit, cuts=(), dtype=jnp.bfloat16):
    drawn = deviation * jax.random.normal(rng, dims, jnp.float32)
    if cuts:
        drawn = drawn * block_levels(rng, dims, cuts, -0.22, 0.18)
    return jnp.clip(drawn, -limit, limit).astype(dtype)


def setup_inputs(seed: int = 0) -> dict:
    seeds = jax.random.split(jax.random.key(seed), 9)
    return {
        "token_ids": touch_ends(skewed_ids(seeds[0], (SEQ,), V, 2), jax.random.fold_in(seeds[0], 3), 0, V - 1).astype(jnp.int32),
        "embed_table": scatter_about(seeds[1], (V, D), 1.0, 6.0),
        "norm_gain": jnp.clip(1.0 + 0.15 * jax.random.normal(seeds[2], (D,), jnp.float32), 0.25, 1.75),
        "w_in": scatter_about(seeds[3], (D, 3, C), D ** -0.5, 0.09375, ((2, 8),)),
        "short_taps": scatter_about(seeds[4], (3, 3, C), 0.6, 3.0, ((2, 8),), jnp.float32),
        "long_filter": scatter_about(seeds[5], (C, SEQ), SEQ ** -0.5, 0.0390625, ((0, 8), (1, 32))),
        "skip_gain": jnp.clip(0.5 + 1.5 * jax.random.uniform(seeds[6], (C,), jnp.float32) ** block_levels(seeds[6], (C,), ((0, 8),), -0.2, 0.2), 0.5, 2.0),
        "w_out": scatter_about(seeds[7], (C, D), C ** -0.5, 0.125, ((1, 8),)),
    }


norm_eps = 1e-06

def causal_conv(pair):
    signal, kernel = pair
    length = signal.shape[-1]
    spectrum = jnp.fft.rfft(signal, n=2 * length, axis=-1) * jnp.fft.rfft(kernel, n=2 * length, axis=-1)
    return jnp.fft.irfft(spectrum, n=2 * length, axis=-1)[:, :length]

def reference(token_ids, embed_table, norm_gain, w_in, short_taps, long_filter, skip_gain, w_out):
    embedded = jnp.take(embed_table, token_ids, axis=0).astype(jnp.float32)
    scale = lax.rsqrt(lax.optimization_barrier(jnp.mean(embedded * embedded, axis=1, keepdims=True)) + norm_eps)
    normed = (embedded * scale * norm_gain).astype(jnp.bfloat16)
    width = normed.shape[1]
    channels = w_in.shape[2]
    projected = jnp.dot(normed.astype(jnp.float32), w_in.reshape(width, 3 * channels).astype(jnp.float32), precision=lax.Precision.HIGHEST, preferred_element_type=jnp.float32)
    projected = lax.optimization_barrier(projected.astype(jnp.bfloat16))
    projected = projected.reshape(-1, 3, channels).astype(jnp.float32)
    once = jnp.pad(projected, ((1, 0), (0, 0), (0, 0)))[:-1]
    twice = jnp.pad(projected, ((2, 0), (0, 0), (0, 0)))[:-2]
    shortened = short_taps[0] * projected + short_taps[1] * once + short_taps[2] * twice
    shortened = lax.optimization_barrier(shortened.astype(jnp.bfloat16)).astype(jnp.float32)
    query = shortened[:, 0, :].T
    key_side = shortened[:, 1, :]
    value_side = shortened[:, 2, :]
    product = lax.optimization_barrier((key_side * value_side).astype(jnp.bfloat16))
    product = product.astype(jnp.float32).T
    length = product.shape[1]
    filters = long_filter.astype(jnp.float32)
    block = 128
    convolved = lax.map(causal_conv, (product.reshape(channels // block, block, length), filters.reshape(channels // block, block, length)))
    convolved = convolved.reshape(channels, length)
    skipped = lax.optimization_barrier((convolved + skip_gain[:, None] * product).astype(jnp.bfloat16))
    gated = (query * skipped.astype(jnp.float32)).astype(jnp.bfloat16)
    gated_rows = gated.astype(jnp.float32).T
    projected_out = jnp.dot(gated_rows, w_out.astype(jnp.float32), precision=lax.Precision.HIGHEST, preferred_element_type=jnp.float32)
    return (embedded + projected_out).astype(jnp.bfloat16)
```

```python
import functools
import math

import jax
import jax.numpy as jnp
import numpy as np
from jax import lax
from jax.experimental import pallas as pl
from jax.experimental.pallas import tpu as pltpu
from jax.sharding import Mesh
from jax.sharding import PartitionSpec as P

CTX = ("x", "zl", "core")
MESH = pl.DeviceIdType.MESH
PEERS = 32
TP = 8
norm_eps = 1e-06


@functools.lru_cache(maxsize=None)
def tables(peers, per):
    R = peers * per
    N = 256 * R
    order = (np.arange(per)[:, None] + per * np.arange(peers)[None, :]).reshape(-1)
    k1 = np.arange(R) + 0.5
    a1 = 2 * np.pi * np.outer(k1, order) / (2 * R)
    f1 = np.concatenate([np.cos(a1), -np.sin(a1)], 0)
    at = 2 * np.pi * np.outer(k1, np.arange(128)) / N
    a2 = 2 * np.pi * (np.outer(np.arange(128), np.arange(128)) % 128) / 128
    c, s = np.cos(a2), np.sin(a2)
    w2 = np.block([[c, -s], [s, c]])
    w2i = np.block([[c, s], [-s, c]])
    f1i = np.concatenate([np.cos(a1.T), -np.sin(a1.T)], 1)
    return f1, np.cos(at), np.sin(at), w2, w2i, f1i


def peer_of(p):
    return {"x": p // 8, "zl": lax.rem(p // 2, 4), "core": lax.rem(p, 2)}


def ctx_index():
    return lax.axis_index("x") * 8 + lax.axis_index("zl") * 2 + lax.axis_index("core")


def exchange_kernel(count, *refs):
    ins, outs, ss, rs = refs[:count], refs[count : 2 * count], refs[2 * count], refs[2 * count + 1]
    me = ctx_index()
    bar = pltpu.get_barrier_semaphore()

    def greet(d, carry):
        pl.semaphore_signal(bar, inc=1, device_id=peer_of(lax.rem(me + d, PEERS)), device_id_type=MESH)
        return carry

    lax.fori_loop(1, PEERS, greet, 0)
    pl.semaphore_wait(bar, PEERS - 1)

    def copy(a, d):
        p = lax.rem(me + d, PEERS)
        return pltpu.make_async_remote_copy(
            src_ref=ins[a].at[p],
            dst_ref=outs[a].at[me],
            send_sem=ss.at[a, d],
            recv_sem=rs.at[a, d],
            device_id=peer_of(p),
            device_id_type=MESH,
        )

    for a in range(count):

        def go(d, carry, a=a):
            copy(a, d).start()
            return carry

        lax.fori_loop(1, PEERS, go, 0)
    for a in range(count):
        outs[a][me] = ins[a][me]

        def done(d, carry, a=a):
            copy(a, d).wait()
            return carry

        lax.fori_loop(1, PEERS, done, 0)


def exchange(arrays, cid):
    count = len(arrays)
    vmem = pl.BlockSpec(memory_space=pltpu.VMEM)
    return pl.pallas_call(
        functools.partial(exchange_kernel, count),
        out_shape=[jax.ShapeDtypeStruct(a.shape, a.dtype) for a in arrays],
        in_specs=[vmem] * count,
        out_specs=[vmem] * count,
        scratch_shapes=[
            pltpu.SemaphoreType.DMA((count, PEERS)),
            pltpu.SemaphoreType.DMA((count, PEERS)),
        ],
        compiler_params=pltpu.CompilerParams(collective_id=cid, has_side_effects=True),
        name=f"exchange_{cid}",
    )(*arrays)


def dot(a, b):
    return jnp.dot(a, b, preferred_element_type=jnp.float32)


def conv_kernel(x_ref, h_ref, gain_ref, f1_ref, ct_ref, st_ref, w2_ref, w2i_ref, f1i_ref, o_ref, flat, xs, spec, back, bs):
    peers, owned, span = x_ref.shape
    per = span // 128
    R = peers * per

    def forward(ref, slot):
        x = ref[...].astype(jnp.float32).reshape(peers * owned, span)
        for q in range(per):
            flat[q * peers * owned : (q + 1) * peers * owned, :] = x[:, q * 128 : (q + 1) * 128]
        for c in range(owned):
            for q in range(per):
                xs[q * peers : (q + 1) * peers, c * 128 : (c + 1) * 128] = flat[
                    pl.ds(q * peers * owned + c, peers, stride=owned), :
                ].astype(jnp.bfloat16)
        ct, st = ct_ref[...], st_ref[...]
        for c2 in range(owned // 2):
            first = dot(f1_ref[...], xs[:, c2 * 256 : (c2 + 1) * 256])
            for half in range(2):
                c = 2 * c2 + half
                re = first[:R, half * 128 : half * 128 + 128]
                im = first[R:, half * 128 : half * 128 + 128]
                rows = pl.ds(c * R, R)
                back[rows, 0:128] = (re * ct + im * st).astype(jnp.bfloat16)
                back[rows, 128:256] = (im * ct - re * st).astype(jnp.bfloat16)
        for c in range(owned):
            rows = pl.ds(c * R, R)
            spec[slot, rows, :] = dot(back[rows, :], w2_ref[...])

    forward(h_ref, 1)
    forward(x_ref, 0)
    ct, st = ct_ref[...], st_ref[...]
    for c in range(owned):
        rows = pl.ds(c * R, R)
        ar, ai = spec[0, rows, 0:128], spec[0, rows, 128:256]
        br, bi = spec[1, rows, 0:128], spec[1, rows, 128:256]
        back[rows, 0:128] = (ar * br - ai * bi).astype(jnp.bfloat16)
        back[rows, 128:256] = (ar * bi + ai * br).astype(jnp.bfloat16)
        u = dot(back[rows, :], w2i_ref[...])
        ur, ui = u[:, 0:128], u[:, 128:256]
        bs[0:R, c * 128 : (c + 1) * 128] = (ur * ct - ui * st).astype(jnp.bfloat16)
        bs[R : 2 * R, c * 128 : (c + 1) * 128] = (ui * ct + ur * st).astype(jnp.bfloat16)
    scale = 2.0 / (256 * R)
    for c2 in range(owned // 2):
        y = dot(f1i_ref[...], bs[:, c2 * 256 : (c2 + 1) * 256]) * scale
        for half in range(2):
            c = 2 * c2 + half
            for q in range(per):
                flat[pl.ds(q * peers * owned + c, peers, stride=owned), :] = y[
                    q * peers : (q + 1) * peers, half * 128 : half * 128 + 128
                ]
    for q in range(per):
        cols = slice(q * 128, (q + 1) * 128)
        x = x_ref[:, :, cols].astype(jnp.float32)
        y = flat[q * peers * owned : (q + 1) * peers * owned, :].reshape(peers, owned, 128)
        o_ref[:, :, cols] = (y + gain_ref[...] * x).astype(jnp.bfloat16)


def long_conv(x, h, gain):
    peers, owned, span = x.shape
    per = span // 128
    R = peers * per
    f1, ct, st, w2, w2i, f1i = tables(peers, per)
    bf = lambda a: jnp.asarray(a.astype(jnp.bfloat16))
    f32 = lambda a: jnp.asarray(a.astype(np.float32))
    vmem = pl.BlockSpec(memory_space=pltpu.VMEM)
    return pl.pallas_call(
        conv_kernel,
        out_shape=jax.ShapeDtypeStruct(x.shape, jnp.bfloat16),
        in_specs=[vmem] * 9,
        out_specs=vmem,
        scratch_shapes=[
            pltpu.VMEM((per * peers * owned, 128), jnp.float32),
            pltpu.VMEM((R, owned * 128), jnp.bfloat16),
            pltpu.VMEM((2, owned * R, 256), jnp.float32),
            pltpu.VMEM((owned * R, 256), jnp.bfloat16),
            pltpu.VMEM((2 * R, owned * 128), jnp.bfloat16),
        ],
        name="long_conv",
    )(x, h, gain, bf(f1), f32(ct), f32(st), bf(w2), bf(w2i), bf(f1i))


CHUNKS = 6


def output_kernel(g_ref, w_ref, res_ref, o_ref, buf, zs, zr, us, ur, ds, dr, ls, lr):
    zh, y = lax.axis_index("zh"), lax.axis_index("y")
    own, other = zh * 4 + y, (1 - zh) * 4 + y
    up, down = lax.rem(y + 1, 4), lax.rem(y + 3, 4)
    T = g_ref.shape[0]
    part = g_ref.shape[1]
    step = T // CHUNKS
    bar = pltpu.get_barrier_semaphore()
    for dev in ({"zh": 1 - zh}, {"y": up}, {"y": down}):
        pl.semaphore_signal(bar, inc=1, device_id=dev, device_id_type=MESH)
    pl.semaphore_wait(bar, 3)

    def send(src, dst, s, r, dev):
        return pltpu.make_async_remote_copy(
            src_ref=src, dst_ref=dst, send_sem=s, recv_sem=r, device_id=dev, device_id_type=MESH
        )

    def rows(c):
        return pl.ds(c * step, step)

    def across(c):
        return send(g_ref.at[rows(c)], buf.at[own, rows(c)], zs.at[c], zr.at[c], {"zh": 1 - zh})

    def slot(k, yy):
        return (zh if k == 0 else 1 - zh) * 4 + yy

    def direct(k, c, upward):
        src = g_ref.at[rows(c)] if k == 0 else buf.at[other, rows(c)]
        s, r = (us, ur) if upward else (ds, dr)
        return send(
            src, buf.at[slot(k, y), rows(c)], s.at[k, c], r.at[k, c], {"y": up if upward else down}
        )

    def relay(k, c):
        upward = c % 2 == 0
        b = slot(k, down if upward else up)
        return send(buf.at[b, rows(c)], buf.at[b, rows(c)], ls.at[k, c], lr.at[k, c], {"y": up if upward else down})

    def forward(k, c):
        upward = c % 2 == 0
        direct(k, c, upward).wait_recv()
        relay(k, c).start()

    def spread(c):
        across(c).wait_recv()
        direct(1, c, True).start()
        direct(1, c, False).start()

    for c in range(CHUNKS):
        across(c).start()
        direct(0, c, True).start()
        direct(0, c, False).start()
    buf[own] = g_ref[...]
    order = []
    for c in range(CHUNKS):
        order.append((forward, (0, c)))
        if c % 2 == 1:
            order.append((spread, ((c - 1) // 2,)))
    for c in range(CHUNKS // 2, CHUNKS):
        order.append((spread, (c,)))
        order.append((forward, (1, c - CHUNKS // 2)))
    for c in range(CHUNKS // 2, CHUNKS):
        order.append((forward, (1, c)))
    for f, a in order:
        f(*a)
    for c in range(CHUNKS):
        for k in range(2):
            direct(k, c, c % 2 == 1).wait_recv()
            relay(k, c).wait_recv()
        acc = res_ref[rows(c), :].astype(jnp.float32)
        for j in range(TP):
            acc += dot(buf[j, rows(c), :], w_ref[j * part : (j + 1) * part, :])
        o_ref[rows(c), :] = acc.astype(jnp.bfloat16)
    for c in range(CHUNKS):
        across(c).wait_send()
        for k in range(2):
            direct(k, c, True).wait_send()
            direct(k, c, False).wait_send()
            relay(k, c).wait_send()


def output(gated, w_out, residual, cid):
    T, part = gated.shape
    vmem = pl.BlockSpec(memory_space=pltpu.VMEM)
    dma = pltpu.SemaphoreType.DMA
    return pl.pallas_call(
        output_kernel,
        out_shape=jax.ShapeDtypeStruct(residual.shape, jnp.bfloat16),
        in_specs=[vmem] * 3,
        out_specs=vmem,
        scratch_shapes=[
            pltpu.VMEM((TP, T, part), jnp.bfloat16),
            dma((CHUNKS,)),
            dma((CHUNKS,)),
            dma((2, CHUNKS)),
            dma((2, CHUNKS)),
            dma((2, CHUNKS)),
            dma((2, CHUNKS)),
            dma((2, CHUNKS)),
            dma((2, CHUNKS)),
        ],
        compiler_params=pltpu.CompilerParams(collective_id=cid, has_side_effects=True),
        name="output",
    )(gated, w_out, residual)


def shifted(block, axis, distance):
    devices = range(lax.axis_size(axis))
    route = [(i - distance, i) for i in devices if i - distance in devices]
    return lax.ppermute(block, axis, route)


def local(token_ids, embed_table, norm_gain, w_in, short_taps, long_filter, skip_gain, w_out):
    vocab = embed_table.shape[0]
    T = token_ids.shape[0]
    chan = w_in.shape[2]
    owned = chan // PEERS
    prior = shifted(token_ids[T - 2 :] + 1, CTX, 1)
    ids = jnp.concatenate([prior, token_ids + 1]) - 1
    table = embed_table.astype(jnp.float32)
    scale = lax.rsqrt(jnp.mean(table * table, axis=1, keepdims=True) + norm_eps)
    normed = (table * scale * norm_gain).astype(jnp.bfloat16)
    w3 = jnp.transpose(w_in, (1, 0, 2))
    rows = [dot(normed, w3[s]).astype(jnp.bfloat16) for s in range(3)]
    hot = (ids[:, None] == jnp.arange(vocab, dtype=jnp.int32)[None, :]).astype(jnp.bfloat16)
    residual = dot(
        hot[2:], lax.dynamic_slice_in_dim(embed_table, (lax.axis_index("zh") * 4 + lax.axis_index("y")) * w_out.shape[1], w_out.shape[1], 1)
    ).astype(jnp.bfloat16)

    def short(s):
        e = lax.dot_general(rows[s], hot, (((0,), (1,)), ((), ())), preferred_element_type=jnp.float32)
        return (
            short_taps[0, s][:, None] * e[:, 2:]
            + short_taps[1, s][:, None] * e[:, 1 : T + 1]
            + short_taps[2, s][:, None] * e[:, 0:T]
        ).astype(jnp.bfloat16)

    query, key, value = short(0), short(1), short(2)
    product = (key.astype(jnp.float32) * value.astype(jnp.float32)).astype(jnp.bfloat16)
    px, ph = exchange([product.reshape(PEERS, owned, T), long_filter.reshape(PEERS, owned, T)], 0)
    own_skip = lax.dynamic_slice_in_dim(skip_gain, ctx_index() * owned, owned)[:, None]
    skipped = long_conv(px, ph, own_skip)
    (returned,) = exchange([skipped], 1)
    returned = returned.reshape(chan, T)
    gated = (query.astype(jnp.float32) * returned.astype(jnp.float32)).astype(jnp.bfloat16).T
    return output(gated, w_out, residual, 2)


def solution(mesh):
    finer = Mesh(mesh.devices.reshape(4, 4, 2, 2, 4), ("x", "zl", "core", "zh", "y"))
    tp = ("zh", "y")
    in_specs = (
        P(CTX),
        P(),
        P(),
        P(None, None, tp),
        P(None, None, tp),
        P(tp, CTX),
        P(tp),
        P(None, tp),
    )
    return jax.shard_map(local, mesh=finer, in_specs=in_specs, out_specs=P(CTX, tp), check_vma=False)
```

```python
import functools
import math

import jax
import jax.numpy as jnp
import numpy as np
from jax import lax
from jax.experimental import pallas as pl
from jax.experimental.pallas import tpu as pltpu
from jax.sharding import Mesh
from jax.sharding import PartitionSpec as P

CTX = ("x", "zl", "core")
MESH = pl.DeviceIdType.MESH
PEERS = 32
TP = 8
norm_eps = 1e-06


@functools.lru_cache(maxsize=None)
def tables(peers, per):
    R = peers * per
    N = 256 * R
    order = (np.arange(per)[:, None] + per * np.arange(peers)[None, :]).reshape(-1)
    k1 = np.arange(R) + 0.5
    a1 = 2 * np.pi * np.outer(k1, order) / (2 * R)
    f1 = np.concatenate([np.cos(a1), -np.sin(a1)], 0)
    at = 2 * np.pi * np.outer(k1, np.arange(128)) / N
    a2 = 2 * np.pi * (np.outer(np.arange(128), np.arange(128)) % 128) / 128
    c, s = np.cos(a2), np.sin(a2)
    w2 = np.block([[c, -s], [s, c]])
    w2i = np.block([[c, s], [-s, c]])
    f1i = np.concatenate([np.cos(a1.T), -np.sin(a1.T)], 1)
    return f1, np.cos(at), np.sin(at), w2, w2i, f1i


def peer_of(p):
    return {"x": p // 8, "zl": lax.rem(p // 2, 4), "core": lax.rem(p, 2)}


def ctx_index():
    return lax.axis_index("x") * 8 + lax.axis_index("zl") * 2 + lax.axis_index("core")


def dot(a, b):
    return jnp.dot(a, b, preferred_element_type=jnp.float32)


def send(src, dst, s, r, dev):
    return pltpu.make_async_remote_copy(
        src_ref=src, dst_ref=dst, send_sem=s, recv_sem=r, device_id=dev, device_id_type=MESH
    )


CHUNKS = 6
HALO = 16


def normalize(tv, gain_ref, nv):
    vocab, width = tv.shape

    @pl.loop(0, vocab // 32)
    def _(r):
        rows = pl.ds(pl.multiple_of(r * 32, 32), 32)
        acc = jnp.zeros((32, 128), jnp.float32)
        for j in range(width // 128):
            x = tv[rows, j * 128 : (j + 1) * 128].astype(jnp.float32)
            acc += x * x
        scale = lax.rsqrt(jnp.sum(acc, axis=1, keepdims=True) * (1.0 / width) + norm_eps)
        for j in range(width // 128):
            cols = slice(j * 128, (j + 1) * 128)
            x = tv[rows, cols].astype(jnp.float32)
            nv[rows, cols] = (x * scale * gain_ref[:, cols]).astype(jnp.bfloat16)


def one_hot(ids_row, vocab):
    column = jnp.transpose(jnp.broadcast_to(ids_row, (128, 128)))
    lane = lax.broadcasted_iota(jnp.int32, (128, 128), 1)
    return [(column == lane + 128 * j) for j in range(vocab // 128)]


def block_kernel(
    ids_ref, gain_ref, taps_ref, skip_ref, ct_ref, st_ref, table_hbm, w3_hbm, filt_hbm, wo_hbm, f1_hbm, w2_hbm, w2i_hbm, f1i_hbm,
    o_ref,
    tv, nv, wv, pv, hot, ev, wo, f1, w2, w2i, f1i, idp, skips, qv, psend, px, hx, res, flat, xs, spec, back, bs, sk, ret, gv, buf,
    ld, ids_s, ids_r, fs, fr, ps, pr, xsnd, xrcv, zs, zr, us, ur, ds, dr, ls, lr,
):
    me = ctx_index()
    zh, y = lax.axis_index("zh"), lax.axis_index("y")
    own, other = zh * 4 + y, (1 - zh) * 4 + y
    up, down = lax.rem(y + 1, 4), lax.rem(y + 3, 4)
    vocab = tv.shape[0]
    T, part = qv.shape
    owned = part // PEERS
    step = T // CHUNKS
    per = T // 128
    R = PEERS * per

    loads = [
        pltpu.make_async_copy(a, b, ld.at[i])
        for i, (a, b) in enumerate(
            [
                (table_hbm, tv),
                (w3_hbm.at[0], wv.at[0]),
                (w3_hbm.at[1], wv.at[1]),
                (w3_hbm.at[2], wv.at[2]),
                (filt_hbm.at[me], hx.at[me]),
                (f1_hbm, f1),
                (w2_hbm, w2),
                (w2i_hbm, w2i),
                (f1i_hbm, f1i),
                (wo_hbm, wo),
            ]
        )
    ]
    for c in loads:
        c.start()

    bar = pltpu.get_barrier_semaphore()
    for dev in ({"zh": 1 - zh}, {"y": up}, {"y": down}):
        pl.semaphore_signal(bar, inc=1, device_id=dev, device_id_type=MESH)

    def greet(d, carry):
        pl.semaphore_signal(bar, inc=1, device_id=peer_of(lax.rem(me + d, PEERS)), device_id_type=MESH)
        return carry

    lax.fori_loop(1, PEERS, greet, 0)
    pl.semaphore_wait(bar, PEERS + 2)

    def to_all(make):
        def go(d, carry):
            make(lax.rem(me + d, PEERS)).start()
            return carry

        lax.fori_loop(1, PEERS, go, 0)

    nxt = lax.rem(me + 1, PEERS)
    ids_copy = send(ids_ref, idp, ids_s, ids_r, peer_of(nxt))
    ids_copy.start()
    to_all(lambda p: send(filt_hbm.at[p], hx.at[me], fs, fr, peer_of(p)))

    def all_of(ref, s, r):
        most = ref.at[pl.ds(0, PEERS - 1)]
        return send(most, most, s, r, peer_of(nxt))

    loads[0].wait()
    normalize(tv, gain_ref, nv)
    for s in range(3):
        loads[1 + s].wait()

    @pl.loop(0, 3)
    def _(s):
        pv[s] = dot(nv[...], wv[s]).astype(jnp.bfloat16)

    for b in range(per):
        for j, hit in enumerate(one_hot(ids_ref[b : b + 1, :], vocab)):
            hot[HALO + b * 128 : HALO + (b + 1) * 128, j * 128 : (j + 1) * 128] = hit.astype(jnp.float32).astype(jnp.bfloat16)
    ids_copy.wait_recv()
    for j, hit in enumerate(one_hot(idp[per - 1 : per, :], vocab)):
        keep = jnp.where(me > 0, hit[128 - HALO :, :].astype(jnp.float32), 0.0)
        hot[0:HALO, j * 128 : (j + 1) * 128] = keep.astype(jnp.bfloat16)
    for s in range(3):
        ev[:, s * part : (s + 1) * part] = dot(hot[...], pv[s])

    def short(s, b):
        cols = slice(s * part, (s + 1) * part)
        at = HALO + b * 128
        out = taps_ref[0, s : s + 1, :] * ev[at : at + 128, cols]
        out += taps_ref[1, s : s + 1, :] * ev[at - 1 : at + 127, cols]
        out += taps_ref[2, s : s + 1, :] * ev[at - 2 : at + 126, cols]
        return out.astype(jnp.bfloat16)

    for b in range(per):
        cols = slice(b * 128, (b + 1) * 128)
        key, value = short(1, b).astype(jnp.float32), short(2, b).astype(jnp.float32)
        psend[:, :, cols] = jnp.transpose(key * value).reshape(PEERS, owned, 128).astype(jnp.bfloat16)
    to_all(lambda p: send(psend.at[p], px.at[me], ps, pr, peer_of(p)))
    px[me] = psend[me]

    for b in range(per):
        qv[b * 128 : (b + 1) * 128, :] = short(0, b)
    width = o_ref.shape[1]
    res[...] = dot(hot[HALO:, :], tv[:, pl.ds(pl.multiple_of(own * width, width), width)]).astype(jnp.bfloat16)
    for j in range(part // 128):
        skips[j * 128 : (j + 1) * 128, :] = jnp.transpose(jnp.broadcast_to(skip_ref[j : j + 1, :], (128, 128)))

    def forward(ref, slot):
        for q in range(per):
            flat[q * PEERS * owned : (q + 1) * PEERS * owned, :] = ref[:, :, q * 128 : (q + 1) * 128].astype(jnp.float32).reshape(PEERS * owned, 128)
        for c in range(owned):
            for q in range(per):
                xs[q * PEERS : (q + 1) * PEERS, c * 128 : (c + 1) * 128] = flat[
                    pl.ds(q * PEERS * owned + c, PEERS, stride=owned), :
                ].astype(jnp.bfloat16)
        ct, st = ct_ref[...], st_ref[...]
        for c2 in range(owned // 2):
            first = dot(f1[...], xs[:, c2 * 256 : (c2 + 1) * 256])
            for half in range(2):
                c = 2 * c2 + half
                re = first[:R, half * 128 : half * 128 + 128]
                im = first[R:, half * 128 : half * 128 + 128]
                rows = slice(c * R, (c + 1) * R)
                back[rows, 0:128] = (re * ct + im * st).astype(jnp.bfloat16)
                back[rows, 128:256] = (im * ct - re * st).astype(jnp.bfloat16)
        for c in range(owned):
            rows = slice(c * R, (c + 1) * R)
            spec[slot, rows, :] = dot(back[rows, :], w2[...])

    for i in range(4, 9):
        loads[i].wait()
    all_of(hx, fs, fr).wait_recv()
    forward(hx, 1)
    all_of(px, ps, pr).wait_recv()
    forward(px, 0)
    ct, st = ct_ref[...], st_ref[...]
    for c in range(owned):
        rows = slice(c * R, (c + 1) * R)
        ar, ai = spec[0, rows, 0:128], spec[0, rows, 128:256]
        br, bi = spec[1, rows, 0:128], spec[1, rows, 128:256]
        back[rows, 0:128] = (ar * br - ai * bi).astype(jnp.bfloat16)
        back[rows, 128:256] = (ar * bi + ai * br).astype(jnp.bfloat16)
        u = dot(back[rows, :], w2i[...])
        ur_, ui_ = u[:, 0:128], u[:, 128:256]
        bs[0:R, c * 128 : (c + 1) * 128] = (ur_ * ct - ui_ * st).astype(jnp.bfloat16)
        bs[R : 2 * R, c * 128 : (c + 1) * 128] = (ui_ * ct + ur_ * st).astype(jnp.bfloat16)
    scale = 2.0 / (256 * R)
    for c2 in range(owned // 2):
        z = dot(f1i[...], bs[:, c2 * 256 : (c2 + 1) * 256]) * scale
        for half in range(2):
            c = 2 * c2 + half
            for q in range(per):
                flat[pl.ds(q * PEERS * owned + c, PEERS, stride=owned), :] = z[
                    q * PEERS : (q + 1) * PEERS, half * 128 : half * 128 + 128
                ]
    direct_gain = skips[pl.ds(pl.multiple_of(me * owned, owned), owned), :]
    for q in range(per):
        cols = slice(q * 128, (q + 1) * 128)
        x = px[:, :, cols].astype(jnp.float32)
        z = flat[q * PEERS * owned : (q + 1) * PEERS * owned, :].reshape(PEERS, owned, 128)
        sk[:, :, cols] = (z + direct_gain[None] * x).astype(jnp.bfloat16)

    def cols_of(q):
        return pl.ds(q * step, step)

    def across(c):
        return send(gv.at[cols_of(c)], buf.at[own, cols_of(c)], zs.at[c], zr.at[c], {"zh": 1 - zh})

    def slot_of(k, yy):
        return (zh if k == 0 else 1 - zh) * 4 + yy

    def direct(k, c, upward):
        src = gv.at[cols_of(c)] if k == 0 else buf.at[other, cols_of(c)]
        s, r = (us, ur) if upward else (ds, dr)
        return send(
            src, buf.at[slot_of(k, y), cols_of(c)], s.at[k, c], r.at[k, c], {"y": up if upward else down}
        )

    def relay(k, c):
        upward = c % 2 == 0
        b = slot_of(k, down if upward else up)
        here = buf.at[b, cols_of(c)]
        return send(here, here, ls.at[k, c], lr.at[k, c], {"y": up if upward else down})

    def returned(q):
        most = ret.at[pl.ds(0, PEERS - 1), :, cols_of(q)]
        return send(most, most, xsnd.at[q], xrcv.at[q], peer_of(nxt))

    def gate(q):
        rows = slice(q * step, (q + 1) * step)
        returned(q).wait_recv()
        arrived = jnp.transpose(ret[:, :, rows].astype(jnp.float32).reshape(part, step))
        gated = (arrived * qv[rows, :].astype(jnp.float32)).astype(jnp.bfloat16)
        gv[rows, :] = gated
        across(q).start()
        direct(0, q, True).start()
        direct(0, q, False).start()
        buf[own, rows, :] = gated

    def pass_on(k, c):
        direct(k, c, c % 2 == 0).wait_recv()
        relay(k, c).start()

    def spread(c):
        across(c).wait_recv()
        direct(1, c, True).start()
        direct(1, c, False).start()

    def finish(c):
        rows = slice(c * step, (c + 1) * step)
        for k in range(2):
            direct(k, c, c % 2 == 1).wait_recv()
            relay(k, c).wait_recv()
        acc = res[rows, :].astype(jnp.float32)
        for j in range(TP):
            acc += dot(buf[j, rows, :], wo[j * part : (j + 1) * part, :])
        o_ref[rows, :] = acc.astype(jnp.bfloat16)

    for q in range(CHUNKS):
        to_all(lambda p: send(sk.at[p, :, cols_of(q)], ret.at[me, :, cols_of(q)], xsnd.at[q], xrcv.at[q], peer_of(p)))
    ret[me] = sk[me]
    loads[9].wait()
    for s in range(CHUNKS + 5):
        for f, lag in ((gate, 0), (lambda c: pass_on(0, c), 1), (spread, 2), (lambda c: pass_on(1, c), 3), (finish, 4)):
            if 0 <= s - lag < CHUNKS:
                f(s - lag)

    ids_copy.wait_send()
    all_of(hx, fs, fr).wait_send()
    all_of(px, ps, pr).wait_send()
    for c in range(CHUNKS):
        returned(c).wait_send()
        across(c).wait_send()
        for k in range(2):
            direct(k, c, True).wait_send()
            direct(k, c, False).wait_send()
            relay(k, c).wait_send()


def local(token_ids, embed_table, norm_gain, w_in, short_taps, long_filter, skip_gain, w_out):
    vocab, width = embed_table.shape
    T = token_ids.shape[0]
    part = w_in.shape[2]
    owned = part // PEERS
    per = T // 128
    R = PEERS * per
    cols = w_out.shape[1]
    f1, ct, st, w2, w2i, f1i = tables(PEERS, per)
    bf = lambda a: jnp.asarray(a.astype(jnp.bfloat16))
    f32 = lambda a: jnp.asarray(a.astype(np.float32))
    vmem = pl.BlockSpec(memory_space=pltpu.VMEM)
    hbm = pl.BlockSpec(memory_space=pl.ANY)
    dma = pltpu.SemaphoreType.DMA
    B, F = jnp.bfloat16, jnp.float32
    V = pltpu.VMEM
    return pl.pallas_call(
        block_kernel,
        out_shape=jax.ShapeDtypeStruct((T, cols), B),
        in_specs=[vmem] * 6 + [hbm] * 8,
        out_specs=vmem,
        scratch_shapes=[
            V((vocab, width), B),
            V((vocab, width), B),
            V((3, width, part), B),
            V((3, vocab, part), B),
            V((HALO + T, vocab), B),
            V((HALO + T, 3 * part), F),
            V(w_out.shape, B),
            V(f1.shape, B),
            V(w2.shape, B),
            V(w2i.shape, B),
            V(f1i.shape, B),
            V((per, 128), jnp.int32),
            V((part, 128), F),
            V((T, part), B),
            V((PEERS, owned, T), B),
            V((PEERS, owned, T), B),
            V((PEERS, owned, T), B),
            V((T, cols), B),
            V((per * part, 128), F),
            V((R, owned * 128), B),
            V((2, owned * R, 256), F),
            V((owned * R, 256), B),
            V((2 * R, owned * 128), B),
            V((PEERS, owned, T), B),
            V((PEERS, owned, T), B),
            V((T, part), B),
            V((TP, T, part), B),
            dma((10,)),
            dma,
            dma,
            dma,
            dma,
            dma,
            dma,
            dma((CHUNKS,)),
            dma((CHUNKS,)),
            dma((CHUNKS,)),
            dma((CHUNKS,)),
        ]
        + [dma((2, CHUNKS))] * 6,
        compiler_params=pltpu.CompilerParams(collective_id=0, has_side_effects=True, vmem_limit_bytes=60 * 2**20),
        name="block",
    )(
        token_ids.reshape(per, 128),
        norm_gain.reshape(1, width),
        short_taps,
        skip_gain.reshape(part // 128, 128),
        f32(ct),
        f32(st),
        embed_table,
        jnp.transpose(w_in, (1, 0, 2)),
        long_filter.reshape(PEERS, owned, T),
        w_out,
        bf(f1),
        bf(w2),
        bf(w2i),
        bf(f1i),
    )


def solution(mesh):
    finer = Mesh(mesh.devices.reshape(4, 4, 2, 2, 4), ("x", "zl", "core", "zh", "y"))
    tp = ("zh", "y")
    in_specs = (
        P(CTX),
        P(),
        P(),
        P(None, None, tp),
        P(None, None, tp),
        P(tp, CTX),
        P(tp),
        P(None, tp),
    )
    return jax.shard_map(local, mesh=finer, in_specs=in_specs, out_specs=P(CTX, tp), check_vma=False)
```

```python
import functools
import math

import jax
import jax.numpy as jnp
import numpy as np
from jax import lax
from jax.experimental import pallas as pl
from jax.experimental.pallas import tpu as pltpu
from jax.sharding import Mesh
from jax.sharding import PartitionSpec as P

CTX = ("x", "zl", "core")
MESH = pl.DeviceIdType.MESH
PEERS = 32
TP = 8
norm_eps = 1e-06


@functools.lru_cache(maxsize=None)
def tables(peers, per):
    R = peers * per
    N = 256 * R
    order = (np.arange(per)[:, None] + per * np.arange(peers)[None, :]).reshape(-1)
    k1 = np.arange(R) + 0.5
    a1 = 2 * np.pi * np.outer(k1, order) / (2 * R)
    f1 = np.concatenate([np.cos(a1), -np.sin(a1)], 0)
    at = 2 * np.pi * np.outer(k1, np.arange(128)) / N
    a2 = 2 * np.pi * (np.outer(np.arange(128), np.arange(128)) % 128) / 128
    c, s = np.cos(a2), np.sin(a2)
    w2 = np.block([[c, -s], [s, c]])
    w2i = np.block([[c, s], [-s, c]])
    f1i = np.concatenate([np.cos(a1.T), -np.sin(a1.T)], 1)
    return f1, np.cos(at), np.sin(at), w2, w2i, f1i


def peer_of(p):
    return {"x": p // 8, "zl": lax.rem(p // 2, 4), "core": lax.rem(p, 2)}


def ctx_index():
    return lax.axis_index("x") * 8 + lax.axis_index("zl") * 2 + lax.axis_index("core")


def dot(a, b):
    return jnp.dot(a, b, preferred_element_type=jnp.float32)


def send(src, dst, s, r, dev):
    return pltpu.make_async_remote_copy(
        src_ref=src, dst_ref=dst, send_sem=s, recv_sem=r, device_id=dev, device_id_type=MESH
    )


CHUNKS = 6
UNROLL = 3
EARLY = 8


def normalize(tv, gain_ref, nv, first, last):
    width = tv.shape[1]

    @pl.loop(first, last)
    def _(r):
        rows = pl.ds(pl.multiple_of(r * 32, 32), 32)
        acc = jnp.zeros((32, 128), jnp.float32)
        for j in range(width // 128):
            x = tv[rows, j * 128 : (j + 1) * 128].astype(jnp.float32)
            acc += x * x
        scale = lax.rsqrt(jnp.sum(acc, axis=1, keepdims=True) * (1.0 / width) + norm_eps)
        for j in range(width // 128):
            cols = slice(j * 128, (j + 1) * 128)
            x = tv[rows, cols].astype(jnp.float32)
            nv[rows, cols] = (x * scale * gain_ref[:, cols]).astype(jnp.bfloat16)


def upright(row):
    return jnp.transpose(jnp.broadcast_to(row, (128, 128)))


def block_kernel(
    ids_ref, gain_ref, taps_ref, skip_ref, ct_ref, st_ref, table_hbm, w3_hbm, filt_hbm, wo_hbm, f1_hbm, w2_hbm, w2i_hbm, f1i_hbm,
    o_ref,
    tv, nv, wv, hot, wo, f1, w2, w2i, f1i, idall, column, small, rows_t, hx, pf, qf, res, flat, xs, spec, back, bs, sk, ret, buf,
    ld, ids_s, ids_r, fs, fr, xsnd, xrcv, us, ur, ds, dr, ls, lr,
):
    x, zl, core = lax.axis_index("x"), lax.axis_index("zl"), lax.axis_index("core")
    me = ctx_index()
    zh, y = lax.axis_index("zh"), lax.axis_index("y")
    own = zh * 4 + y
    up, down = lax.rem(y + 1, 4), lax.rem(y + 3, 4)
    vocab = tv.shape[0]
    part = small.shape[1]
    T = res.shape[0]
    owned = part // PEERS
    step = T // CHUNKS
    per = T // 128
    R = PEERS * per
    half, inside = me // 16, pl.multiple_of(lax.rem(me, 16) * owned, owned)

    def each_peer(planes, fn):
        def chip(t, skip_self):
            px, pz = lax.rem(x + t // 4, 4), lax.rem(zl + lax.rem(t, 4), 4)
            for dc in range(2):
                pc = lax.rem(core + dc, 2)
                p = px * 8 + pz * 2 + pc
                for k in range(planes):
                    if not (skip_self and dc == 0 and k == 0):
                        dev = {"x": px, "zl": pz, "core": pc}
                        if k == 1:
                            dev["zh"] = 1 - zh
                        fn(p, k, dev)

        def go(t, carry):
            chip(t, False)
            return carry

        lax.fori_loop(1, 16, go, 0, unroll=UNROLL)
        chip(0, True)

    bar = pltpu.get_barrier_semaphore()

    def greet(dev):
        pl.semaphore_signal(bar, inc=1, device_id=dev, device_id_type=MESH)

    each_peer(2, lambda p, k, dev: greet(dev))
    greet({"y": up})
    greet({"y": down})

    loads = [
        pltpu.make_async_copy(a, b, ld.at[i])
        for i, (a, b) in enumerate(
            [(table_hbm, tv)]
            + [(w3_hbm.at[s, :, pl.ds(pl.multiple_of(half * 128, 128), 128)], wv.at[:, pl.ds(s * 128, 128)]) for s in range(3)]
            + [(filt_hbm.at[me], hx.at[me]), (f1_hbm, f1), (w2_hbm, w2), (w2i_hbm, w2i), (f1i_hbm, f1i), (wo_hbm, wo)]
        )
    ]
    for c in loads:
        c.start()

    for r in range(3):
        for s in range(3):
            row = jnp.where(half == 0, taps_ref[r, s : s + 1, 0:128], taps_ref[r, s : s + 1, 128:256])
            column[...] = upright(row)
            rows_t[r * 3 + s] = column[pl.ds(inside, owned), :]
    column[...] = upright(jnp.where(half == 0, skip_ref[0:1, :], skip_ref[1:2, :]))
    rows_t[9] = column[pl.ds(inside, owned), :]
    idall[me] = ids_ref[...]
    loads[0].wait()
    normalize(tv, gain_ref, nv, 0, EARLY)

    pl.semaphore_wait(bar, 2 * PEERS + 1)

    each_peer(1, lambda p, k, dev: send(ids_ref, idall.at[me], ids_s, ids_r, dev).start())
    each_peer(1, lambda p, k, dev: send(filt_hbm.at[p], hx.at[me], fs, fr, dev).start())

    def all_of(ref, s, r):
        most = ref.at[pl.ds(0, PEERS - 1)]
        return send(most, most, s, r, {"y": up})

    normalize(tv, gain_ref, nv, EARLY, vocab // 32)
    for s in range(3):
        loads[1 + s].wait()
    table_rows = []
    for n0, n1 in ((0, 256), (256, 384)):
        projected = dot(nv[...], wv[:, n0:n1]).astype(jnp.bfloat16).astype(jnp.float32)
        for n in range(n0, n1, 128):
            for v in range(vocab // 128):
                flat[v * 128 : (v + 1) * 128, :] = jnp.transpose(projected[v * 128 : (v + 1) * 128, n - n0 : n - n0 + 128])
            table_rows.append(
                jnp.concatenate([flat[pl.ds(pl.multiple_of(v * 128 + inside, owned), owned), :] for v in range(vocab // 128)], axis=1)
            )
    picks = jnp.concatenate(table_rows, axis=0).astype(jnp.bfloat16)

    all_of(idall, ids_s, ids_r).wait_recv()
    lane = lax.broadcasted_iota(jnp.int32, (owned, 128), 1)
    token = lax.broadcasted_iota(jnp.int32, (vocab, 128), 0)

    def positions(i, carry):
        for q2 in range(per // 2):
            hits = [
                (jnp.broadcast_to(idall[i, q : q + 1, :], (vocab, 128)) == token).astype(jnp.float32).astype(jnp.bfloat16)
                for q in (2 * q2, 2 * q2 + 1)
            ]
            chosen = dot(picks, jnp.concatenate(hits, axis=1))
            for h in range(2):
                q = 2 * q2 + h
                short, later = [], []
                for s in range(3):
                    now = chosen[s * owned : (s + 1) * owned, h * 128 : (h + 1) * 128]
                    by1, by2 = pltpu.roll(now, 1, 1), pltpu.roll(now, 2, 1)
                    before1, before2 = carry[s]
                    one = jnp.where(lane < 1, before1, by1)
                    two = jnp.where(lane < 2, before2, by2)
                    short.append(
                        (rows_t[s] * now + rows_t[3 + s] * one + rows_t[6 + s] * two).astype(jnp.bfloat16).astype(jnp.float32)
                    )
                    later.append((by1, by2))
                carry = tuple(later)
                rows = pl.ds(pl.multiple_of(q * part + i * owned, owned), owned)
                pf[rows, :] = (short[1] * short[2]).astype(jnp.bfloat16).astype(jnp.float32)
                qf[rows, :] = short[0]
        return carry

    nothing = jnp.zeros((owned, 128), jnp.float32)
    lax.fori_loop(0, PEERS, positions, ((nothing, nothing),) * 3, unroll=4)

    def forward(src, slot):
        for c in range(owned):
            for q in range(per):
                xs[q * PEERS : (q + 1) * PEERS, c * 128 : (c + 1) * 128] = src[
                    pl.ds(q * part + c, PEERS, stride=owned), :
                ].astype(jnp.bfloat16)
        ct, st = ct_ref[...], st_ref[...]
        for c2 in range(owned // 2):
            first = dot(f1[...], xs[:, c2 * 256 : (c2 + 1) * 256])
            for h in range(2):
                c = 2 * c2 + h
                re = first[:R, h * 128 : h * 128 + 128]
                im = first[R:, h * 128 : h * 128 + 128]
                rows = slice(c * R, (c + 1) * R)
                back[rows, 0:128] = (re * ct + im * st).astype(jnp.bfloat16)
                back[rows, 128:256] = (im * ct - re * st).astype(jnp.bfloat16)
        for c in range(owned):
            rows = slice(c * R, (c + 1) * R)
            spec[slot, rows, :] = dot(back[rows, :], w2[...])

    for i in range(4, 9):
        loads[i].wait()
    forward(pf, 0)
    all_of(hx, fs, fr).wait_recv()
    for q in range(per):
        flat[q * part : (q + 1) * part, :] = hx[:, :, q * 128 : (q + 1) * 128].astype(jnp.float32).reshape(part, 128)
    forward(flat, 1)
    ct, st = ct_ref[...], st_ref[...]
    for c in range(owned):
        rows = slice(c * R, (c + 1) * R)
        ar, ai = spec[0, rows, 0:128], spec[0, rows, 128:256]
        br, bi = spec[1, rows, 0:128], spec[1, rows, 128:256]
        back[rows, 0:128] = (ar * br - ai * bi).astype(jnp.bfloat16)
        back[rows, 128:256] = (ar * bi + ai * br).astype(jnp.bfloat16)
        u = dot(back[rows, :], w2i[...])
        ur_, ui_ = u[:, 0:128], u[:, 128:256]
        bs[0:R, c * 128 : (c + 1) * 128] = (ur_ * ct - ui_ * st).astype(jnp.bfloat16)
        bs[R : 2 * R, c * 128 : (c + 1) * 128] = (ui_ * ct + ur_ * st).astype(jnp.bfloat16)
    scale = 2.0 / (256 * R)
    for c2 in range(owned // 2):
        z = dot(f1i[...], bs[:, c2 * 256 : (c2 + 1) * 256]) * scale
        for h in range(2):
            c = 2 * c2 + h
            for q in range(per):
                flat[pl.ds(q * part + c, PEERS, stride=owned), :] = z[q * PEERS : (q + 1) * PEERS, h * 128 : h * 128 + 128]

    def cols_of(q):
        return pl.ds(q * step, step)

    for q in range(CHUNKS):
        rows = slice(q * part, (q + 1) * part)
        gain = jnp.broadcast_to(rows_t[9][None], (PEERS, owned, 128)).reshape(part, 128)
        skipped = (flat[rows, :] + gain * pf[rows, :]).astype(jnp.bfloat16).astype(jnp.float32)
        gated = (qf[rows, :] * skipped).astype(jnp.bfloat16)
        sk[:, :, q * step : (q + 1) * step] = gated.reshape(PEERS, owned, 128)
        each_peer(
            2, lambda p, k, dev: send(sk.at[p, :, cols_of(q)], ret.at[k, me, :, cols_of(q)], xsnd.at[k, q], xrcv.at[k, q], dev).start()
        )
        ret[0, me, :, q * step : (q + 1) * step] = sk[me, :, q * step : (q + 1) * step]

    lanes = lax.broadcasted_iota(jnp.int32, (128, 128), 1)
    for b in range(per):
        col = upright(ids_ref[b : b + 1, :])
        for j in range(vocab // 128):
            hot[b * 128 : (b + 1) * 128, j * 128 : (j + 1) * 128] = (col == lanes + 128 * j).astype(jnp.float32).astype(jnp.bfloat16)
    width = o_ref.shape[1]
    res[...] = dot(hot[...], tv[:, pl.ds(pl.multiple_of(own * width, width), width)]).astype(jnp.bfloat16)
    loads[9].wait()

    def slot_of(k, yy):
        return (zh if k == 0 else 1 - zh) * 4 + yy

    def direct(k, c, upward):
        here = buf.at[slot_of(k, y), cols_of(c)]
        s, r = (us, ur) if upward else (ds, dr)
        return send(here, here, s.at[k, c], r.at[k, c], {"y": up if upward else down})

    def relay(k, c):
        upward = (c + k) % 2 == 0
        here = buf.at[slot_of(k, down if upward else up), cols_of(c)]
        return send(here, here, ls.at[k, c], lr.at[k, c], {"y": up if upward else down})

    def returned(k, q):
        most = ret.at[k, pl.ds(0, PEERS - 1 + k), :, cols_of(q)]
        return send(most, most, xsnd.at[k, q], xrcv.at[k, q], {"y": up})

    def turn(k, q):
        returned(k, q).wait_recv()
        rows = slice(q * step, (q + 1) * step)
        arrived = ret[k, :, :, rows].astype(jnp.float32).reshape(part, step)
        buf[slot_of(k, y), rows, :] = jnp.transpose(arrived).astype(jnp.bfloat16)
        direct(k, q, True).start()
        direct(k, q, False).start()

    def pass_on(k, c):
        direct(k, c, (c + k) % 2 == 0).wait_recv()
        relay(k, c).start()

    def finish(c):
        rows = slice(c * step, (c + 1) * step)
        for k in range(2):
            direct(k, c, (c + k) % 2 == 1).wait_recv()
            relay(k, c).wait_recv()
        acc = res[rows, :].astype(jnp.float32)
        for j in range(TP):
            acc += dot(buf[j, rows, :], wo[j * part : (j + 1) * part, :])
        o_ref[rows, :] = acc.astype(jnp.bfloat16)

    for s in range(CHUNKS + 3):
        for k in range(2):
            if s < CHUNKS:
                turn(k, s)
            if 0 <= s - 1 < CHUNKS:
                pass_on(k, s - 1)
        if 0 <= s - 3 < CHUNKS:
            finish(s - 3)

    all_of(idall, ids_s, ids_r).wait_send()
    all_of(hx, fs, fr).wait_send()
    for c in range(CHUNKS):
        for k in range(2):
            returned(k, c).wait_send()
            direct(k, c, True).wait_send()
            direct(k, c, False).wait_send()
            relay(k, c).wait_send()


def local(token_ids, embed_table, norm_gain, w_in, short_taps, long_filter, skip_gain, w_out):
    vocab, width = embed_table.shape
    T = token_ids.shape[0]
    part = w_in.shape[2]
    owned = part // PEERS
    per = T // 128
    R = PEERS * per
    cols = w_out.shape[1]
    f1, ct, st, w2, w2i, f1i = tables(PEERS, per)
    bf = lambda a: jnp.asarray(a.astype(jnp.bfloat16))
    f32 = lambda a: jnp.asarray(a.astype(np.float32))
    vmem = pl.BlockSpec(memory_space=pltpu.VMEM)
    hbm = pl.BlockSpec(memory_space=pl.ANY)
    dma = pltpu.SemaphoreType.DMA
    B, F = jnp.bfloat16, jnp.float32
    V = pltpu.VMEM
    return pl.pallas_call(
        block_kernel,
        out_shape=jax.ShapeDtypeStruct((T, cols), B),
        in_specs=[vmem] * 6 + [hbm] * 8,
        out_specs=vmem,
        scratch_shapes=[
            V((vocab, width), B),
            V((vocab, width), B),
            V((width, 384), B),
            V((T, vocab), B),
            V(w_out.shape, B),
            V(f1.shape, B),
            V(w2.shape, B),
            V(w2i.shape, B),
            V(f1i.shape, B),
            V((PEERS, per, 128), jnp.int32),
            V((128, 128), F),
            V((8, part), F),
            V((10, owned, 128), F),
            V((PEERS, owned, T), B),
            V((per * part, 128), F),
            V((per * part, 128), F),
            V((T, cols), B),
            V((per * part, 128), F),
            V((R, owned * 128), B),
            V((2, owned * R, 256), F),
            V((owned * R, 256), B),
            V((2 * R, owned * 128), B),
            V((PEERS, owned, T), B),
            V((2, PEERS, owned, T), B),
            V((TP, T, part), B),
            dma((10,)),
            dma,
            dma,
            dma,
            dma,
        ]
        + [dma((2, CHUNKS))] * 8,
        compiler_params=pltpu.CompilerParams(collective_id=0, has_side_effects=True, vmem_limit_bytes=60 * 2**20),
        name="block",
    )(
        token_ids.reshape(per, 128),
        norm_gain.reshape(1, width),
        short_taps,
        skip_gain.reshape(part // 128, 128),
        f32(ct),
        f32(st),
        embed_table,
        jnp.transpose(w_in, (1, 0, 2)),
        long_filter.reshape(PEERS, owned, T),
        w_out,
        bf(f1),
        bf(w2),
        bf(w2i),
        bf(f1i),
    )


def solution(mesh):
    finer = Mesh(mesh.devices.reshape(4, 4, 2, 2, 4), ("x", "zl", "core", "zh", "y"))
    tp = ("zh", "y")
    in_specs = (
        P(CTX),
        P(),
        P(),
        P(None, None, tp),
        P(None, None, tp),
        P(tp, CTX),
        P(tp),
        P(None, tp),
    )
    return jax.shard_map(local, mesh=finer, in_specs=in_specs, out_specs=P(CTX, tp), check_vma=False)
```

```python
import functools
import math

import jax
import jax.numpy as jnp
import numpy as np
from jax import lax
from jax.experimental import pallas as pl
from jax.experimental.pallas import tpu as pltpu
from jax.sharding import Mesh
from jax.sharding import PartitionSpec as P

CTX = ("x", "zl", "core")
MESH = pl.DeviceIdType.MESH
PEERS = 32
TP = 8
norm_eps = 1e-06


@functools.lru_cache(maxsize=None)
def tables(peers, per):
    R = peers * per
    N = 256 * R
    order = (np.arange(per)[:, None] + per * np.arange(peers)[None, :]).reshape(-1)
    k1 = np.arange(R) + 0.5
    a1 = 2 * np.pi * np.outer(k1, order) / (2 * R)
    f1 = np.concatenate([np.cos(a1), -np.sin(a1)], 0)
    at = 2 * np.pi * np.outer(k1, np.arange(128)) / N
    a2 = 2 * np.pi * (np.outer(np.arange(128), np.arange(128)) % 128) / 128
    c, s = np.cos(a2), np.sin(a2)
    w2 = np.block([[c, -s], [s, c]])
    w2i = np.block([[c, s], [-s, c]])
    f1i = np.concatenate([np.cos(a1.T), -np.sin(a1.T)], 1)
    return f1, np.cos(at), np.sin(at), w2, w2i, f1i


def peer_of(p):
    return {"x": p // 8, "zl": lax.rem(p // 2, 4), "core": lax.rem(p, 2)}


def ctx_index():
    return lax.axis_index("x") * 8 + lax.axis_index("zl") * 2 + lax.axis_index("core")


def dot(a, b):
    return jnp.dot(a, b, preferred_element_type=jnp.float32)


def send(src, dst, s, r, dev):
    return pltpu.make_async_remote_copy(
        src_ref=src, dst_ref=dst, send_sem=s, recv_sem=r, device_id=dev, device_id_type=MESH
    )


CHUNKS = 6
UNROLL = 3
EARLY = 8


def normalize(tv, gain_ref, nv, first, last):
    width = tv.shape[1]

    @pl.loop(first, last)
    def _(r):
        rows = pl.ds(pl.multiple_of(r * 32, 32), 32)
        acc = jnp.zeros((32, 128), jnp.float32)
        for j in range(width // 128):
            x = tv[rows, j * 128 : (j + 1) * 128].astype(jnp.float32)
            acc += x * x
        scale = lax.rsqrt(jnp.sum(acc, axis=1, keepdims=True) * (1.0 / width) + norm_eps)
        for j in range(width // 128):
            cols = slice(j * 128, (j + 1) * 128)
            x = tv[rows, cols].astype(jnp.float32)
            nv[rows, cols] = (x * scale * gain_ref[:, cols]).astype(jnp.bfloat16)


def upright(row):
    return jnp.transpose(jnp.broadcast_to(row, (128, 128)))


def block_kernel(
    ids_hbm, gain_hbm, taps_hbm, skip_hbm, ct_hbm, st_hbm, table_hbm, w3_hbm, filt_hbm, wo_hbm, f1_hbm, w2_hbm, w2i_hbm, f1i_hbm,
    o_ref,
    ids_ref, gain_ref, taps_ref, skip_ref, ct_ref, st_ref, fv, tv, nv, wv, hot, wo, f1, w2, w2i, f1i, idall, column, small, rows_t, hx, pf, qf, res, flat, xs, spec, back, bs, sk, ret, buf,
    ld, ids_s, ids_r, fs, fr, xsnd, xrcv, us, ur, ds, dr, ls, lr,
):
    x, zl, core = lax.axis_index("x"), lax.axis_index("zl"), lax.axis_index("core")
    me = ctx_index()
    zh, y = lax.axis_index("zh"), lax.axis_index("y")
    own = zh * 4 + y
    up, down = lax.rem(y + 1, 4), lax.rem(y + 3, 4)
    vocab = tv.shape[0]
    part = small.shape[1]
    T = res.shape[0]
    owned = part // PEERS
    step = T // CHUNKS
    per = T // 128
    R = PEERS * per
    half, inside = me // 16, pl.multiple_of(lax.rem(me, 16) * owned, owned)

    def each_peer(planes, fn):
        def chip(t, skip_self):
            px, pz = lax.rem(x + t // 4, 4), lax.rem(zl + lax.rem(t, 4), 4)
            for dc in range(2):
                pc = lax.rem(core + dc, 2)
                p = px * 8 + pz * 2 + pc
                for k in range(planes):
                    if not (skip_self and dc == 0 and k == 0):
                        dev = {"x": px, "zl": pz, "core": pc}
                        if k == 1:
                            dev["zh"] = 1 - zh
                        fn(p, k, dev)

        def go(t, carry):
            chip(t, False)
            return carry

        lax.fori_loop(1, 16, go, 0, unroll=UNROLL)
        chip(0, True)

    bar = pltpu.get_barrier_semaphore()

    def greet(dev):
        pl.semaphore_signal(bar, inc=1, device_id=dev, device_id_type=MESH)

    each_peer(2, lambda p, k, dev: greet(dev))
    greet({"y": up})
    greet({"y": down})

    loads = [
        pltpu.make_async_copy(a, b, ld.at[i])
        for i, (a, b) in enumerate(
            [(table_hbm, tv), (gain_hbm, gain_ref), (ids_hbm, ids_ref), (filt_hbm, fv), (taps_hbm, taps_ref), (skip_hbm, skip_ref)]
            + [(w3_hbm.at[s, :, pl.ds(pl.multiple_of(half * 128, 128), 128)], wv.at[:, pl.ds(s * 128, 128)]) for s in range(3)]
            + [(ct_hbm, ct_ref), (st_hbm, st_ref), (f1_hbm, f1), (w2_hbm, w2), (w2i_hbm, w2i), (f1i_hbm, f1i), (wo_hbm, wo)]
        )
    ]
    for c in loads:
        c.start()

    for i in range(2):
        loads[i].wait()
    normalize(tv, gain_ref, nv, 0, EARLY)
    for i in range(2, 4):
        loads[i].wait()

    pl.semaphore_wait(bar, 2 * PEERS + 1)

    each_peer(1, lambda p, k, dev: send(ids_ref, idall.at[me], ids_s, ids_r, dev).start())
    each_peer(1, lambda p, k, dev: send(fv.at[p], hx.at[me], fs, fr, dev).start())

    def all_of(ref, s, r):
        most = ref.at[pl.ds(0, PEERS - 1)]
        return send(most, most, s, r, {"y": up})

    idall[me] = ids_ref[...]
    hx[me] = fv[me]
    for i in range(4, 6):
        loads[i].wait()

    for r in range(3):
        for s in range(3):
            row = jnp.where(half == 0, taps_ref[r, s : s + 1, 0:128], taps_ref[r, s : s + 1, 128:256])
            column[...] = upright(row)
            rows_t[r * 3 + s] = column[pl.ds(inside, owned), :]
    column[...] = upright(jnp.where(half == 0, skip_ref[0:1, :], skip_ref[1:2, :]))
    rows_t[9] = column[pl.ds(inside, owned), :]
    normalize(tv, gain_ref, nv, EARLY, vocab // 32)
    for s in range(3):
        loads[6 + s].wait()
    table_rows = []
    for n0, n1 in ((0, 256), (256, 384)):
        projected = dot(nv[...], wv[:, n0:n1]).astype(jnp.bfloat16).astype(jnp.float32)
        for n in range(n0, n1, 128):
            for v in range(vocab // 128):
                flat[v * 128 : (v + 1) * 128, :] = jnp.transpose(projected[v * 128 : (v + 1) * 128, n - n0 : n - n0 + 128])
            table_rows.append([flat[pl.ds(pl.multiple_of(v * 128 + inside, owned), owned), :] for v in range(vocab // 128)])
    groups = vocab // 128
    picks = jnp.concatenate([table_rows[s][v] for v in range(groups) for s in range(3)], axis=0).astype(jnp.bfloat16)

    all_of(idall, ids_s, ids_r).wait_recv()
    lane = lax.broadcasted_iota(jnp.int32, (owned, 128), 1)
    token = lax.broadcasted_iota(jnp.int32, (128, 128), 0)

    def positions(i, carry):
        for q2 in range(per // 2):
            pair = [idall[i, q : q + 1, :] for q in (2 * q2, 2 * q2 + 1)]
            hits = [(jnp.broadcast_to(ids & 127, (128, 128)) == token).astype(jnp.float32).astype(jnp.bfloat16) for ids in pair]
            chosen = dot(picks, jnp.concatenate(hits, axis=1))
            for h in range(2):
                q = 2 * q2 + h
                group = jnp.broadcast_to(pair[h] >> 7, (owned, 128))
                short, later = [], []
                for s in range(3):
                    of = [
                        chosen[(v * 3 + s) * owned : (v * 3 + s + 1) * owned, h * 128 : (h + 1) * 128] for v in range(groups)
                    ]
                    now = of[0]
                    for v in range(1, groups):
                        now = jnp.where(group == v, of[v], now)
                    by1, by2 = pltpu.roll(now, 1, 1), pltpu.roll(now, 2, 1)
                    before1, before2 = carry[s]
                    one = jnp.where(lane < 1, before1, by1)
                    two = jnp.where(lane < 2, before2, by2)
                    short.append(
                        (rows_t[s] * now + rows_t[3 + s] * one + rows_t[6 + s] * two).astype(jnp.bfloat16).astype(jnp.float32)
                    )
                    later.append((by1, by2))
                carry = tuple(later)
                rows = pl.ds(pl.multiple_of(q * part + i * owned, owned), owned)
                pf[rows, :] = (short[1] * short[2]).astype(jnp.bfloat16).astype(jnp.float32)
                qf[rows, :] = short[0]
        return carry

    nothing = jnp.zeros((owned, 128), jnp.float32)
    lax.fori_loop(0, PEERS, positions, ((nothing, nothing),) * 3, unroll=4)

    def forward(src, slot):
        for c in range(owned):
            for q in range(per):
                xs[q * PEERS : (q + 1) * PEERS, c * 128 : (c + 1) * 128] = src[
                    pl.ds(q * part + c, PEERS, stride=owned), :
                ].astype(jnp.bfloat16)
        ct, st = ct_ref[...], st_ref[...]
        for c2 in range(owned // 2):
            first = dot(f1[...], xs[:, c2 * 256 : (c2 + 1) * 256])
            for h in range(2):
                c = 2 * c2 + h
                re = first[:R, h * 128 : h * 128 + 128]
                im = first[R:, h * 128 : h * 128 + 128]
                rows = slice(c * R, (c + 1) * R)
                back[rows, 0:128] = (re * ct + im * st).astype(jnp.bfloat16)
                back[rows, 128:256] = (im * ct - re * st).astype(jnp.bfloat16)
        for c in range(owned):
            rows = slice(c * R, (c + 1) * R)
            spec[slot, rows, :] = dot(back[rows, :], w2[...])

    for i in range(9, 15):
        loads[i].wait()
    forward(pf, 0)
    all_of(hx, fs, fr).wait_recv()
    for q in range(per):
        flat[q * part : (q + 1) * part, :] = hx[:, :, q * 128 : (q + 1) * 128].astype(jnp.float32).reshape(part, 128)
    forward(flat, 1)
    ct, st = ct_ref[...], st_ref[...]
    for c in range(owned):
        rows = slice(c * R, (c + 1) * R)
        ar, ai = spec[0, rows, 0:128], spec[0, rows, 128:256]
        br, bi = spec[1, rows, 0:128], spec[1, rows, 128:256]
        back[rows, 0:128] = (ar * br - ai * bi).astype(jnp.bfloat16)
        back[rows, 128:256] = (ar * bi + ai * br).astype(jnp.bfloat16)
        u = dot(back[rows, :], w2i[...])
        ur_, ui_ = u[:, 0:128], u[:, 128:256]
        bs[0:R, c * 128 : (c + 1) * 128] = (ur_ * ct - ui_ * st).astype(jnp.bfloat16)
        bs[R : 2 * R, c * 128 : (c + 1) * 128] = (ui_ * ct + ur_ * st).astype(jnp.bfloat16)
    scale = 2.0 / (256 * R)
    for c2 in range(owned // 2):
        z = dot(f1i[...], bs[:, c2 * 256 : (c2 + 1) * 256]) * scale
        for h in range(2):
            c = 2 * c2 + h
            for q in range(per):
                flat[pl.ds(q * part + c, PEERS, stride=owned), :] = z[q * PEERS : (q + 1) * PEERS, h * 128 : h * 128 + 128]

    def cols_of(q):
        return pl.ds(q * step, step)

    for q in range(CHUNKS):
        rows = slice(q * part, (q + 1) * part)
        gain = jnp.broadcast_to(rows_t[9][None], (PEERS, owned, 128)).reshape(part, 128)
        skipped = (flat[rows, :] + gain * pf[rows, :]).astype(jnp.bfloat16).astype(jnp.float32)
        gated = (qf[rows, :] * skipped).astype(jnp.bfloat16)
        sk[:, :, q * step : (q + 1) * step] = gated.reshape(PEERS, owned, 128)
        each_peer(
            2, lambda p, k, dev: send(sk.at[p, :, cols_of(q)], ret.at[k, me, :, cols_of(q)], xsnd.at[k, q], xrcv.at[k, q], dev).start()
        )
        ret[0, me, :, q * step : (q + 1) * step] = sk[me, :, q * step : (q + 1) * step]

    lanes = lax.broadcasted_iota(jnp.int32, (128, 128), 1)
    for b in range(per):
        col = upright(ids_ref[b : b + 1, :])
        for j in range(vocab // 128):
            hot[b * 128 : (b + 1) * 128, j * 128 : (j + 1) * 128] = (col == lanes + 128 * j).astype(jnp.float32).astype(jnp.bfloat16)
    width = o_ref.shape[1]
    res[...] = dot(hot[...], tv[:, pl.ds(pl.multiple_of(own * width, width), width)]).astype(jnp.bfloat16)
    loads[15].wait()

    def slot_of(k, yy):
        return (zh if k == 0 else 1 - zh) * 4 + yy

    def direct(k, c, upward):
        here = buf.at[slot_of(k, y), cols_of(c)]
        s, r = (us, ur) if upward else (ds, dr)
        return send(here, here, s.at[k, c], r.at[k, c], {"y": up if upward else down})

    def relay(k, c):
        upward = (c + k) % 2 == 0
        here = buf.at[slot_of(k, down if upward else up), cols_of(c)]
        return send(here, here, ls.at[k, c], lr.at[k, c], {"y": up if upward else down})

    def returned(k, q):
        most = ret.at[k, pl.ds(0, PEERS - 1 + k), :, cols_of(q)]
        return send(most, most, xsnd.at[k, q], xrcv.at[k, q], {"y": up})

    def turn(k, q):
        returned(k, q).wait_recv()
        rows = slice(q * step, (q + 1) * step)
        arrived = ret[k, :, :, rows].astype(jnp.float32).reshape(part, step)
        buf[slot_of(k, y), rows, :] = jnp.transpose(arrived).astype(jnp.bfloat16)
        direct(k, q, True).start()
        direct(k, q, False).start()

    def pass_on(k, c):
        direct(k, c, (c + k) % 2 == 0).wait_recv()
        relay(k, c).start()

    def finish(c):
        rows = slice(c * step, (c + 1) * step)
        for k in range(2):
            direct(k, c, (c + k) % 2 == 1).wait_recv()
            relay(k, c).wait_recv()
        acc = res[rows, :].astype(jnp.float32)
        for j in range(TP):
            acc += dot(buf[j, rows, :], wo[j * part : (j + 1) * part, :])
        o_ref[rows, :] = acc.astype(jnp.bfloat16)

    for s in range(CHUNKS + 3):
        for k in range(2):
            if s < CHUNKS:
                turn(k, s)
            if 0 <= s - 1 < CHUNKS:
                pass_on(k, s - 1)
        if 0 <= s - 3 < CHUNKS:
            finish(s - 3)

    all_of(idall, ids_s, ids_r).wait_send()
    all_of(hx, fs, fr).wait_send()
    for c in range(CHUNKS):
        for k in range(2):
            returned(k, c).wait_send()
            direct(k, c, True).wait_send()
            direct(k, c, False).wait_send()
            relay(k, c).wait_send()


def local(token_ids, embed_table, norm_gain, w_in, short_taps, long_filter, skip_gain, w_out):
    vocab, width = embed_table.shape
    T = token_ids.shape[0]
    part = w_in.shape[2]
    owned = part // PEERS
    per = T // 128
    R = PEERS * per
    cols = w_out.shape[1]
    f1, ct, st, w2, w2i, f1i = tables(PEERS, per)
    bf = lambda a: jnp.asarray(a.astype(jnp.bfloat16))
    f32 = lambda a: jnp.asarray(a.astype(np.float32))
    vmem = pl.BlockSpec(memory_space=pltpu.VMEM)
    hbm = pl.BlockSpec(memory_space=pl.ANY)
    dma = pltpu.SemaphoreType.DMA
    B, F = jnp.bfloat16, jnp.float32
    V = pltpu.VMEM
    return pl.pallas_call(
        block_kernel,
        out_shape=jax.ShapeDtypeStruct((T, cols), B),
        in_specs=[hbm] * 14,
        out_specs=vmem,
        scratch_shapes=[
            V((per, 128), jnp.int32),
            V((1, width), F),
            V(short_taps.shape, F),
            V((part // 128, 128), F),
            V(ct.shape, F),
            V(st.shape, F),
            V((PEERS, owned, T), B),
            V((vocab, width), B),
            V((vocab, width), B),
            V((width, 384), B),
            V((T, vocab), B),
            V(w_out.shape, B),
            V(f1.shape, B),
            V(w2.shape, B),
            V(w2i.shape, B),
            V(f1i.shape, B),
            V((PEERS, per, 128), jnp.int32),
            V((128, 128), F),
            V((8, part), F),
            V((10, owned, 128), F),
            V((PEERS, owned, T), B),
            V((per * part, 128), F),
            V((per * part, 128), F),
            V((T, cols), B),
            V((per * part, 128), F),
            V((R, owned * 128), B),
            V((2, owned * R, 256), F),
            V((owned * R, 256), B),
            V((2 * R, owned * 128), B),
            V((PEERS, owned, T), B),
            V((2, PEERS, owned, T), B),
            V((TP, T, part), B),
            dma((16,)),
            dma,
            dma,
            dma,
            dma,
        ]
        + [dma((2, CHUNKS))] * 8,
        compiler_params=pltpu.CompilerParams(collective_id=0, has_side_effects=True, vmem_limit_bytes=60 * 2**20),
        name="block",
    )(
        token_ids.reshape(per, 128),
        norm_gain.reshape(1, width),
        short_taps,
        skip_gain.reshape(part // 128, 128),
        f32(ct),
        f32(st),
        embed_table,
        jnp.transpose(w_in, (1, 0, 2)),
        long_filter.reshape(PEERS, owned, T),
        w_out,
        bf(f1),
        bf(w2),
        bf(w2i),
        bf(f1i),
    )


def solution(mesh):
    finer = Mesh(mesh.devices.reshape(4, 4, 2, 2, 4), ("x", "zl", "core", "zh", "y"))
    tp = ("zh", "y")
    in_specs = (
        P(CTX),
        P(),
        P(),
        P(None, None, tp),
        P(None, None, tp),
        P(tp, CTX),
        P(tp),
        P(None, tp),
    )
    return jax.shard_map(local, mesh=finer, in_specs=in_specs, out_specs=P(CTX, tp), check_vma=False)
```

```python
import functools
import math

import jax
import jax.numpy as jnp
import numpy as np
from jax import lax
from jax.experimental import pallas as pl
from jax.experimental.pallas import tpu as pltpu
from jax.sharding import Mesh
from jax.sharding import PartitionSpec as P

CTX = ("x", "zl", "core")
MESH = pl.DeviceIdType.MESH
PEERS = 32
TP = 8
norm_eps = 1e-06


@functools.lru_cache(maxsize=None)
def tables(peers, per):
    R = peers * per
    N = 256 * R
    order = (np.arange(per)[:, None] + per * np.arange(peers)[None, :]).reshape(-1)
    k1 = np.arange(R) + 0.5
    a1 = 2 * np.pi * np.outer(k1, order) / (2 * R)
    f1 = np.concatenate([np.cos(a1), -np.sin(a1)], 0)
    at = 2 * np.pi * np.outer(k1, np.arange(128)) / N
    a2 = 2 * np.pi * (np.outer(np.arange(128), np.arange(128)) % 128) / 128
    c, s = np.cos(a2), np.sin(a2)
    w2 = np.block([[c, -s], [s, c]])
    w2i = np.block([[c, s], [-s, c]])
    f1i = np.concatenate([np.cos(a1.T), -np.sin(a1.T)], 1)
    return f1, np.cos(at), np.sin(at), w2, w2i, f1i


def peer_of(p):
    return {"x": p // 8, "zl": lax.rem(p // 2, 4), "core": lax.rem(p, 2)}


def ctx_index():
    return lax.axis_index("x") * 8 + lax.axis_index("zl") * 2 + lax.axis_index("core")


def dot(a, b):
    return jnp.dot(a, b, preferred_element_type=jnp.float32)


def send(src, dst, s, r, dev):
    return pltpu.make_async_remote_copy(
        src_ref=src, dst_ref=dst, send_sem=s, recv_sem=r, device_id=dev, device_id_type=MESH
    )


CHUNKS = 6
UNROLL = 3


def normalize(tv, gain_ref, nv, first, last):
    width = tv.shape[1]

    @pl.loop(first, last)
    def _(r):
        rows = pl.ds(pl.multiple_of(r * 32, 32), 32)
        acc = jnp.zeros((32, 128), jnp.float32)
        for j in range(width // 128):
            x = tv[rows, j * 128 : (j + 1) * 128].astype(jnp.float32)
            acc += x * x
        scale = lax.rsqrt(jnp.sum(acc, axis=1, keepdims=True) * (1.0 / width) + norm_eps)
        for j in range(width // 128):
            cols = slice(j * 128, (j + 1) * 128)
            x = tv[rows, cols].astype(jnp.float32)
            nv[rows, cols] = (x * scale * gain_ref[:, cols]).astype(jnp.bfloat16)


def upright(row):
    return jnp.transpose(jnp.broadcast_to(row, (128, 128)))


def block_kernel(
    ids_hbm, gain_hbm, taps_hbm, skip_hbm, ct_hbm, st_hbm, table_hbm, w3_hbm, filt_hbm, wo_hbm, f1_hbm, w2_hbm, w2i_hbm, f1i_hbm,
    o_ref,
    ids_ref, gain_ref, taps_ref, skip_ref, ct_ref, st_ref, fv, tv, nv, wv, hot, wo, f1, w2, w2i, f1i, idpair, idall, column, small, rows_t, hx, pf, qf, res, flat, xs, spec, back, bs, sk, ret, buf,
    ld, ids_s, ids_r, fs, fr, xsnd, xrcv, us, ur, ds, dr, ls, lr,
):
    x, zl, core = lax.axis_index("x"), lax.axis_index("zl"), lax.axis_index("core")
    me = ctx_index()
    zh, y = lax.axis_index("zh"), lax.axis_index("y")
    own = zh * 4 + y
    up, down = lax.rem(y + 1, 4), lax.rem(y + 3, 4)
    vocab = tv.shape[0]
    part = small.shape[1]
    T = res.shape[0]
    owned = part // PEERS
    step = T // CHUNKS
    per = T // 128
    R = PEERS * per
    half, inside = me // 16, pl.multiple_of(lax.rem(me, 16) * owned, owned)

    def each_peer(planes, fn):
        planes = range(planes) if isinstance(planes, int) else planes

        def chip(t, skip_self):
            px, pz = lax.rem(x + t // 4, 4), lax.rem(zl + lax.rem(t, 4), 4)
            for dc in range(2):
                pc = lax.rem(core + dc, 2)
                p = px * 8 + pz * 2 + pc
                for k in planes:
                    if not (skip_self and dc == 0 and k == 0):
                        dev = {"x": px, "zl": pz, "core": pc}
                        if k == 1:
                            dev["zh"] = 1 - zh
                        fn(p, k, dev)

        def go(t, carry):
            chip(t, False)
            return carry

        lax.fori_loop(1, 16, go, 0, unroll=UNROLL)
        chip(0, True)

    bar = pltpu.get_barrier_semaphore()

    def greet(dev):
        pl.semaphore_signal(bar, inc=1, device_id=dev, device_id_type=MESH)

    each_peer(2, lambda p, k, dev: greet(dev))
    greet({"y": up})
    greet({"y": down})

    loads = [
        pltpu.make_async_copy(a, b, ld.at[i])
        for i, (a, b) in enumerate(
            [(ids_hbm, ids_ref), (filt_hbm, fv), (table_hbm, tv), (gain_hbm, gain_ref), (taps_hbm, taps_ref), (skip_hbm, skip_ref)]
            + [(w3_hbm.at[s, :, pl.ds(pl.multiple_of(half * 128, 128), 128)], wv.at[:, pl.ds(s * 128, 128)]) for s in range(3)]
            + [(ct_hbm, ct_ref), (st_hbm, st_ref), (f1_hbm, f1), (w2_hbm, w2), (w2i_hbm, w2i), (f1i_hbm, f1i), (wo_hbm, wo)]
        )
    ]
    for c in loads:
        c.start()

    for i in range(2):
        loads[i].wait()
    idpair[...] = ids_ref[0 : per // 2, :] + ids_ref[per // 2 : per, :] * 65536
    pl.semaphore_wait(bar, 2 * PEERS + 1)

    each_peer(1, lambda p, k, dev: send(idpair, idall.at[me], ids_s, ids_r, dev).start())
    each_peer(1, lambda p, k, dev: send(fv.at[p], hx.at[me], fs, fr, dev).start())

    def all_of(ref, s, r):
        most = ref.at[pl.ds(0, PEERS - 1)]
        return send(most, most, s, r, {"y": up})

    idall[me] = idpair[...]
    hx[me] = fv[me]
    for i in range(4, 6):
        loads[i].wait()

    for r in range(3):
        for s in range(3):
            row = jnp.where(half == 0, taps_ref[r, s : s + 1, 0:128], taps_ref[r, s : s + 1, 128:256])
            column[...] = upright(row)
            rows_t[r * 3 + s] = column[pl.ds(inside, owned), :]
    column[...] = upright(jnp.where(half == 0, skip_ref[0:1, :], skip_ref[1:2, :]))
    rows_t[9] = column[pl.ds(inside, owned), :]
    for i in range(2, 4):
        loads[i].wait()
    normalize(tv, gain_ref, nv, 0, vocab // 32)
    for s in range(3):
        loads[6 + s].wait()
    table_rows = []
    for n0, n1 in ((0, 256), (256, 384)):
        projected = dot(nv[...], wv[:, n0:n1]).astype(jnp.bfloat16).astype(jnp.float32)
        for n in range(n0, n1, 128):
            for v in range(vocab // 128):
                flat[v * 128 : (v + 1) * 128, :] = jnp.transpose(projected[v * 128 : (v + 1) * 128, n - n0 : n - n0 + 128])
            table_rows.append([flat[pl.ds(pl.multiple_of(v * 128 + inside, owned), owned), :] for v in range(vocab // 128)])
    groups = vocab // 128
    picks = jnp.concatenate([table_rows[s][v] for v in range(groups) for s in range(3)], axis=0).astype(jnp.bfloat16)

    all_of(idall, ids_s, ids_r).wait_recv()
    lane = lax.broadcasted_iota(jnp.int32, (owned, 128), 1)
    token = lax.broadcasted_iota(jnp.int32, (128, 128), 0)

    def positions(i, carry):
        for q2 in range(per // 2):
            pair = [idall[i, q % (per // 2) : q % (per // 2) + 1, :] for q in (2 * q2, 2 * q2 + 1)]
            pair = [ids & 65535 if 2 * q2 + h < per // 2 else ids >> 16 for h, ids in enumerate(pair)]
            hits = [(jnp.broadcast_to(ids & 127, (128, 128)) == token).astype(jnp.float32).astype(jnp.bfloat16) for ids in pair]
            chosen = dot(picks, jnp.concatenate(hits, axis=1))
            for h in range(2):
                q = 2 * q2 + h
                group = jnp.broadcast_to(pair[h] >> 7, (owned, 128))
                short, later = [], []
                for s in range(3):
                    of = [
                        chosen[(v * 3 + s) * owned : (v * 3 + s + 1) * owned, h * 128 : (h + 1) * 128] for v in range(groups)
                    ]
                    now = of[0]
                    for v in range(1, groups):
                        now = jnp.where(group == v, of[v], now)
                    by1, by2 = pltpu.roll(now, 1, 1), pltpu.roll(now, 2, 1)
                    before1, before2 = carry[s]
                    one = jnp.where(lane < 1, before1, by1)
                    two = jnp.where(lane < 2, before2, by2)
                    short.append(
                        (rows_t[s] * now + rows_t[3 + s] * one + rows_t[6 + s] * two).astype(jnp.bfloat16).astype(jnp.float32)
                    )
                    later.append((by1, by2))
                carry = tuple(later)
                rows = pl.ds(pl.multiple_of(q * part + i * owned, owned), owned)
                pf[rows, :] = (short[1] * short[2]).astype(jnp.bfloat16).astype(jnp.float32)
                qf[rows, :] = short[0]
        return carry

    nothing = jnp.zeros((owned, 128), jnp.float32)
    lax.fori_loop(0, PEERS, positions, ((nothing, nothing),) * 3, unroll=4)

    def forward(src, slot):
        for c in range(owned):
            for q in range(per):
                xs[q * PEERS : (q + 1) * PEERS, c * 128 : (c + 1) * 128] = src[
                    pl.ds(q * part + c, PEERS, stride=owned), :
                ].astype(jnp.bfloat16)
        ct, st = ct_ref[...], st_ref[...]
        for c2 in range(owned // 2):
            first = dot(f1[...], xs[:, c2 * 256 : (c2 + 1) * 256])
            for h in range(2):
                c = 2 * c2 + h
                re = first[:R, h * 128 : h * 128 + 128]
                im = first[R:, h * 128 : h * 128 + 128]
                rows = slice(c * R, (c + 1) * R)
                back[rows, 0:128] = (re * ct + im * st).astype(jnp.bfloat16)
                back[rows, 128:256] = (im * ct - re * st).astype(jnp.bfloat16)
        for c in range(owned):
            rows = slice(c * R, (c + 1) * R)
            spec[slot, rows, :] = dot(back[rows, :], w2[...])

    for i in range(9, 15):
        loads[i].wait()
    forward(pf, 0)
    all_of(hx, fs, fr).wait_recv()
    for q in range(per):
        flat[q * part : (q + 1) * part, :] = hx[:, :, q * 128 : (q + 1) * 128].astype(jnp.float32).reshape(part, 128)
    forward(flat, 1)
    ct, st = ct_ref[...], st_ref[...]
    for c in range(owned):
        rows = slice(c * R, (c + 1) * R)
        ar, ai = spec[0, rows, 0:128], spec[0, rows, 128:256]
        br, bi = spec[1, rows, 0:128], spec[1, rows, 128:256]
        back[rows, 0:128] = (ar * br - ai * bi).astype(jnp.bfloat16)
        back[rows, 128:256] = (ar * bi + ai * br).astype(jnp.bfloat16)
        u = dot(back[rows, :], w2i[...])
        ur_, ui_ = u[:, 0:128], u[:, 128:256]
        bs[0:R, c * 128 : (c + 1) * 128] = (ur_ * ct - ui_ * st).astype(jnp.bfloat16)
        bs[R : 2 * R, c * 128 : (c + 1) * 128] = (ui_ * ct + ur_ * st).astype(jnp.bfloat16)
    scale = 2.0 / (256 * R)
    for c2 in range(owned // 2):
        z = dot(f1i[...], bs[:, c2 * 256 : (c2 + 1) * 256]) * scale
        for h in range(2):
            c = 2 * c2 + h
            for q in range(per):
                flat[pl.ds(q * part + c, PEERS, stride=owned), :] = z[q * PEERS : (q + 1) * PEERS, h * 128 : h * 128 + 128]

    def cols_of(q):
        return pl.ds(q * step, step)

    for q in range(CHUNKS):
        rows = slice(q * part, (q + 1) * part)
        gain = jnp.broadcast_to(rows_t[9][None], (PEERS, owned, 128)).reshape(part, 128)
        skipped = (flat[rows, :] + gain * pf[rows, :]).astype(jnp.bfloat16).astype(jnp.float32)
        gated = (qf[rows, :] * skipped).astype(jnp.bfloat16)
        sk[:, :, q * step : (q + 1) * step] = gated.reshape(PEERS, owned, 128)
        for plane in range(2):
            each_peer(
                (plane,),
                lambda p, k, dev: send(sk.at[p, :, cols_of(q)], ret.at[k, me, :, cols_of(q)], xsnd.at[k, q], xrcv.at[k, q], dev).start(),
            )
        ret[0, me, :, q * step : (q + 1) * step] = sk[me, :, q * step : (q + 1) * step]

    lanes = lax.broadcasted_iota(jnp.int32, (128, 128), 1)
    for b in range(per):
        col = upright(ids_ref[b : b + 1, :])
        for j in range(vocab // 128):
            hot[b * 128 : (b + 1) * 128, j * 128 : (j + 1) * 128] = (col == lanes + 128 * j).astype(jnp.float32).astype(jnp.bfloat16)
    width = o_ref.shape[1]
    res[...] = dot(hot[...], tv[:, pl.ds(pl.multiple_of(own * width, width), width)]).astype(jnp.bfloat16)
    loads[15].wait()

    def slot_of(k, yy):
        return (zh if k == 0 else 1 - zh) * 4 + yy

    def direct(k, c, upward):
        here = buf.at[slot_of(k, y), cols_of(c)]
        s, r = (us, ur) if upward else (ds, dr)
        return send(here, here, s.at[k, c], r.at[k, c], {"y": up if upward else down})

    def relay(k, c):
        upward = (c + k) % 2 == 0
        here = buf.at[slot_of(k, down if upward else up), cols_of(c)]
        return send(here, here, ls.at[k, c], lr.at[k, c], {"y": up if upward else down})

    def returned(k, q):
        most = ret.at[k, pl.ds(0, PEERS - 1 + k), :, cols_of(q)]
        return send(most, most, xsnd.at[k, q], xrcv.at[k, q], {"y": up})

    def turn(k, q):
        returned(k, q).wait_recv()
        rows = slice(q * step, (q + 1) * step)
        arrived = ret[k, :, :, rows].astype(jnp.float32).reshape(part, step)
        buf[slot_of(k, y), rows, :] = jnp.transpose(arrived).astype(jnp.bfloat16)
        direct(k, q, True).start()
        direct(k, q, False).start()

    def pass_on(k, c):
        direct(k, c, (c + k) % 2 == 0).wait_recv()
        relay(k, c).start()

    def finish(c):
        rows = slice(c * step, (c + 1) * step)
        for k in range(2):
            direct(k, c, (c + k) % 2 == 1).wait_recv()
            relay(k, c).wait_recv()
        acc = res[rows, :].astype(jnp.float32)
        for j in range(TP):
            acc += dot(buf[j, rows, :], wo[j * part : (j + 1) * part, :])
        o_ref[rows, :] = acc.astype(jnp.bfloat16)

    for s in range(CHUNKS + 3):
        for k in range(2):
            if s < CHUNKS:
                turn(k, s)
            if 0 <= s - 1 < CHUNKS:
                pass_on(k, s - 1)
        if 0 <= s - 3 < CHUNKS:
            finish(s - 3)

    all_of(idall, ids_s, ids_r).wait_send()
    all_of(hx, fs, fr).wait_send()
    for c in range(CHUNKS):
        for k in range(2):
            returned(k, c).wait_send()
            direct(k, c, True).wait_send()
            direct(k, c, False).wait_send()
            relay(k, c).wait_send()


def local(token_ids, embed_table, norm_gain, w_in, short_taps, long_filter, skip_gain, w_out):
    vocab, width = embed_table.shape
    T = token_ids.shape[0]
    part = w_in.shape[2]
    owned = part // PEERS
    per = T // 128
    R = PEERS * per
    cols = w_out.shape[1]
    f1, ct, st, w2, w2i, f1i = tables(PEERS, per)
    bf = lambda a: jnp.asarray(a.astype(jnp.bfloat16))
    f32 = lambda a: jnp.asarray(a.astype(np.float32))
    vmem = pl.BlockSpec(memory_space=pltpu.VMEM)
    hbm = pl.BlockSpec(memory_space=pltpu.HBM)
    dma = pltpu.SemaphoreType.DMA
    B, F = jnp.bfloat16, jnp.float32
    V = pltpu.VMEM
    operands = (
        token_ids.reshape(per, 128),
        norm_gain.reshape(1, width),
        short_taps,
        skip_gain.reshape(part // 128, 128),
        f32(ct),
        f32(st),
        embed_table,
        jnp.transpose(w_in, (1, 0, 2)),
        long_filter.reshape(PEERS, owned, T),
        w_out,
        bf(f1),
        bf(w2),
        bf(w2i),
        bf(f1i),
    )
    return pl.pallas_call(
        block_kernel,
        out_shape=jax.ShapeDtypeStruct((T, cols), B),
        in_specs=[hbm] * 14,
        out_specs=vmem,
        scratch_shapes=[
            V((per, 128), jnp.int32),
            V((1, width), F),
            V(short_taps.shape, F),
            V((part // 128, 128), F),
            V(ct.shape, F),
            V(st.shape, F),
            V((PEERS, owned, T), B),
            V((vocab, width), B),
            V((vocab, width), B),
            V((width, 384), B),
            V((T, vocab), B),
            V(w_out.shape, B),
            V(f1.shape, B),
            V(w2.shape, B),
            V(w2i.shape, B),
            V(f1i.shape, B),
            V((per // 2, 128), jnp.int32),
            V((PEERS, per // 2, 128), jnp.int32),
            V((128, 128), F),
            V((8, part), F),
            V((10, owned, 128), F),
            V((PEERS, owned, T), B),
            V((per * part, 128), F),
            V((per * part, 128), F),
            V((T, cols), B),
            V((per * part, 128), F),
            V((R, owned * 128), B),
            V((2, owned * R, 256), F),
            V((owned * R, 256), B),
            V((2 * R, owned * 128), B),
            V((PEERS, owned, T), B),
            V((2, PEERS, owned, T), B),
            V((TP, T, part), B),
            dma((16,)),
            dma,
            dma,
            dma,
            dma,
        ]
        + [dma((2, CHUNKS))] * 8,
        compiler_params=pltpu.CompilerParams(collective_id=0, has_side_effects=True, vmem_limit_bytes=48 * 2**20),
        name="block",
    )(*(pltpu.with_memory_space_constraint(a, pltpu.HBM) for a in operands))


def solution(mesh):
    finer = Mesh(mesh.devices.reshape(4, 4, 2, 2, 4), ("x", "zl", "core", "zh", "y"))
    tp = ("zh", "y")
    in_specs = (
        P(CTX),
        P(),
        P(),
        P(None, None, tp),
        P(None, None, tp),
        P(tp, CTX),
        P(tp),
        P(None, tp),
    )
    return jax.shard_map(local, mesh=finer, in_specs=in_specs, out_specs=P(CTX, tp), check_vma=False)
```

```python
import functools
import math

import jax
import jax.numpy as jnp
import numpy as np
from jax import lax
from jax.experimental import pallas as pl
from jax.experimental.pallas import tpu as pltpu
from jax.sharding import Mesh
from jax.sharding import PartitionSpec as P

CTX = ("x", "zl", "core")
MESH = pl.DeviceIdType.MESH
PEERS = 32
TP = 8
norm_eps = 1e-06


@functools.lru_cache(maxsize=None)
def tables(peers, per):
    R = peers * per
    N = 256 * R
    order = (np.arange(per)[:, None] + per * np.arange(peers)[None, :]).reshape(-1)
    k1 = np.arange(R) + 0.5
    a1 = 2 * np.pi * np.outer(k1, order) / (2 * R)
    f1 = np.concatenate([np.cos(a1), -np.sin(a1)], 0)
    at = 2 * np.pi * np.outer(k1, np.arange(128)) / N
    a2 = 2 * np.pi * (np.outer(np.arange(128), np.arange(128)) % 128) / 128
    c, s = np.cos(a2), np.sin(a2)
    w2 = np.block([[c, -s], [s, c]])
    w2i = np.block([[c, s], [-s, c]])
    f1i = np.concatenate([np.cos(a1.T), -np.sin(a1.T)], 1)
    return f1, np.cos(at), np.sin(at), w2, w2i, f1i


def peer_of(p):
    return {"x": p // 8, "zl": lax.rem(p // 2, 4), "core": lax.rem(p, 2)}


def ctx_index():
    return lax.axis_index("x") * 8 + lax.axis_index("zl") * 2 + lax.axis_index("core")


def dot(a, b):
    return jnp.dot(a, b, preferred_element_type=jnp.float32)


def send(src, dst, s, r, dev):
    return pltpu.make_async_remote_copy(
        src_ref=src, dst_ref=dst, send_sem=s, recv_sem=r, device_id=dev, device_id_type=MESH
    )


SPANS = 3
UNROLL = 3


def normalize(tv, gain_ref, nv, first, last):
    width = tv.shape[1]

    @pl.loop(first, last)
    def _(r):
        rows = pl.ds(pl.multiple_of(r * 32, 32), 32)
        acc = jnp.zeros((32, 128), jnp.float32)
        for j in range(width // 128):
            x = tv[rows, j * 128 : (j + 1) * 128].astype(jnp.float32)
            acc += x * x
        scale = lax.rsqrt(jnp.sum(acc, axis=1, keepdims=True) * (1.0 / width) + norm_eps)
        for j in range(width // 128):
            cols = slice(j * 128, (j + 1) * 128)
            x = tv[rows, cols].astype(jnp.float32)
            nv[rows, cols] = (x * scale * gain_ref[:, cols]).astype(jnp.bfloat16)


def upright(row):
    return jnp.transpose(jnp.broadcast_to(row, (128, 128)))


def block_kernel(
    ids_hbm, gain_hbm, taps_hbm, skip_hbm, ct_hbm, st_hbm, table_hbm, w3_hbm, filt_hbm, wo_hbm, f1_hbm, w2_hbm, w2i_hbm, f1i_hbm,
    o_ref,
    ids_ref, gain_ref, taps_ref, skip_ref, ct_ref, st_ref, fv, tv, nv, wv, rt, halves, picks, hot, wo, f1, w2, w2i, f1i, idpair, idall, column, rows_t, hx, pf, qf, res, flat, xs, spec, back, bs, sk, ret, buf,
    ld, ids_s, ids_r, fs, fr, pk_s, pk_r, xsnd, xrcv, us, ur, ds, dr, ls, lr,
):
    x, zl, core = lax.axis_index("x"), lax.axis_index("zl"), lax.axis_index("core")
    me = ctx_index()
    zh, y = lax.axis_index("zh"), lax.axis_index("y")
    own = zh * 4 + y
    up, down = lax.rem(y + 1, 4), lax.rem(y + 3, 4)
    mine = tv.shape[0]
    vocab = 2 * mine
    part = fv.shape[0] * fv.shape[1]
    width = o_ref.shape[1]
    T = res.shape[0]
    owned = part // PEERS
    step = T // SPANS
    per = T // 128
    R = PEERS * per
    chip = x * 4 + zl
    block = core * 16 + chip
    inside = pl.multiple_of(chip * owned, owned)

    def at(px, pz, pc, plane):
        dev = {"x": px, "zl": pz, "core": pc}
        if plane == 1:
            dev["zh"] = 1 - zh
        return px * 8 + pz * 2 + pc, pc * 16 + px * 4 + pz, dev

    def each_peer(fn, cores=(0, 1), plane=0, home=True):
        if home and plane == 0:
            fn(*at(x, zl, 1 - core, 0))
        if home and plane == 1:
            for pc in cores:
                fn(*at(x, zl, pc, 1))

        def go(t, carry):
            for pc in cores:
                fn(*at(lax.rem(x + t // 4, 4), lax.rem(zl + lax.rem(t, 4), 4), pc, plane))
            return carry

        lax.fori_loop(1, 16, go, 0, unroll=UNROLL)

    bar = pltpu.get_barrier_semaphore()

    def greet(dev):
        pl.semaphore_signal(bar, inc=1, device_id=dev, device_id_type=MESH)

    for plane in range(2):
        each_peer(lambda p, b, dev: greet(dev), plane=plane)
    greet({"y": up})
    greet({"y": down})

    loads = [
        pltpu.make_async_copy(a, b, ld.at[i])
        for i, (a, b) in enumerate(
            [
                (ids_hbm, ids_ref),
                (filt_hbm, fv),
                (table_hbm.at[pl.ds(pl.multiple_of(core * mine, mine), mine)], tv),
                (gain_hbm, gain_ref),
                (taps_hbm, taps_ref),
                (skip_hbm, skip_ref),
                (w3_hbm.at[0], wv.at[:, pl.ds(0, part)]),
                (w3_hbm.at[1], wv.at[:, pl.ds(part, part)]),
                (w3_hbm.at[2], wv.at[:, pl.ds(2 * part, part)]),
                (ct_hbm, ct_ref),
                (st_hbm, st_ref),
                (f1_hbm, f1),
                (w2_hbm, w2),
                (w2i_hbm, w2i),
                (f1i_hbm, f1i),
                (table_hbm.at[:, pl.ds(pl.multiple_of(own * width, width), width)], rt),
                (wo_hbm.at[:, 0], wo.at[0]),
                (wo_hbm.at[:, 1], wo.at[1]),
            ]
        )
    ]
    for c in loads:
        c.start()

    for i in range(2):
        loads[i].wait()
    idpair[...] = ids_ref[0 : per // 2, :] + ids_ref[per // 2 : per, :] * 65536
    pl.semaphore_wait(bar, 2 * PEERS + 1)

    each_peer(lambda p, b, dev: send(idpair, idall.at[me], ids_s, ids_r, dev).start())
    for pc in range(2):
        each_peer(lambda p, b, dev: send(fv.at[b], hx.at[me], fs, fr, dev).start(), cores=(pc,), home=pc == 0)

    def all_of(ref, s, r):
        most = ref.at[pl.ds(0, PEERS - 1)]
        return send(most, most, s, r, {"y": up})

    idall[me] = idpair[...]
    hx[me] = fv[block]
    for i in range(4, 6):
        loads[i].wait()

    for r in range(3):
        for s in range(3):
            row = jnp.where(core == 0, taps_ref[r, s : s + 1, 0:128], taps_ref[r, s : s + 1, 128:256])
            column[...] = upright(row)
            rows_t[r * 3 + s] = column[pl.ds(inside, owned), :]
    column[...] = upright(jnp.where(core == 0, skip_ref[0:1, :], skip_ref[1:2, :]))
    rows_t[9] = column[pl.ds(inside, owned), :]
    for i in range(2, 4):
        loads[i].wait()
    normalize(tv, gain_ref, nv, 0, mine // 32)
    for s in range(3):
        loads[6 + s].wait()
    for s in range(3):
        projected = dot(nv[...], wv[:, s * part : (s + 1) * part]).astype(jnp.bfloat16).astype(jnp.float32)
        for h in range(2):
            for v in range(mine // 128):
                at_ = ((s * 2 + h) * 2 + v) * 128
                flat[at_ : at_ + 128, :] = jnp.transpose(projected[v * 128 : (v + 1) * 128, h * 128 : (h + 1) * 128])
    for h in range(2):
        for v in range(mine // 128):
            rows = [flat[pl.ds(pl.multiple_of(((s * 2 + h) * 2 + v) * 128 + inside, owned), owned), :] for s in range(3)]
            rows.append(jnp.zeros((owned, 128), jnp.float32))
            halves[h, v] = jnp.concatenate(rows, axis=0).astype(jnp.bfloat16)
    picks_copy = send(halves.at[1 - core], picks.at[pl.ds(2 * core, 2)], pk_s, pk_r, {"core": 1 - core})
    picks_copy.start()
    picks[pl.ds(2 * core, 2)] = halves[core]
    groups = vocab // 128

    all_of(idall, ids_s, ids_r).wait_recv()
    picks_copy.wait_recv()
    table_rows = picks[...].reshape(groups * 4 * owned, 128)
    lane = lax.broadcasted_iota(jnp.int32, (owned, 128), 1)
    token = lax.broadcasted_iota(jnp.int32, (128, 128), 0)

    def positions(i, carry):
        for q2 in range(per // 2):
            pair = [idall[i, q % (per // 2) : q % (per // 2) + 1, :] for q in (2 * q2, 2 * q2 + 1)]
            pair = [ids & 65535 if 2 * q2 + h < per // 2 else ids >> 16 for h, ids in enumerate(pair)]
            hits = [(jnp.broadcast_to(ids & 127, (128, 128)) == token).astype(jnp.float32).astype(jnp.bfloat16) for ids in pair]
            chosen = dot(table_rows, jnp.concatenate(hits, axis=1))
            for h in range(2):
                q = 2 * q2 + h
                group = jnp.broadcast_to(pair[h] >> 7, (owned, 128))
                short, later = [], []
                for s in range(3):
                    of = [
                        chosen[(v * 4 + s) * owned : (v * 4 + s + 1) * owned, h * 128 : (h + 1) * 128] for v in range(groups)
                    ]
                    now = of[0]
                    for v in range(1, groups):
                        now = jnp.where(group == v, of[v], now)
                    by1, by2 = pltpu.roll(now, 1, 1), pltpu.roll(now, 2, 1)
                    before1, before2 = carry[s]
                    one = jnp.where(lane < 1, before1, by1)
                    two = jnp.where(lane < 2, before2, by2)
                    short.append(
                        (rows_t[s] * now + rows_t[3 + s] * one + rows_t[6 + s] * two).astype(jnp.bfloat16).astype(jnp.float32)
                    )
                    later.append((by1, by2))
                carry = tuple(later)
                rows = pl.ds(pl.multiple_of(q * part + i * owned, owned), owned)
                pf[rows, :] = (short[1] * short[2]).astype(jnp.bfloat16).astype(jnp.float32)
                qf[rows, :] = short[0]
        return carry

    nothing = jnp.zeros((owned, 128), jnp.float32)
    lax.fori_loop(0, PEERS, positions, ((nothing, nothing),) * 3, unroll=4)

    def forward(src, slot):
        for c in range(owned):
            for q in range(per):
                xs[q * PEERS : (q + 1) * PEERS, c * 128 : (c + 1) * 128] = src[
                    pl.ds(q * part + c, PEERS, stride=owned), :
                ].astype(jnp.bfloat16)
        ct, st = ct_ref[...], st_ref[...]
        for c2 in range(owned // 2):
            first = dot(f1[...], xs[:, c2 * 256 : (c2 + 1) * 256])
            for h in range(2):
                c = 2 * c2 + h
                re = first[:R, h * 128 : h * 128 + 128]
                im = first[R:, h * 128 : h * 128 + 128]
                rows = slice(c * R, (c + 1) * R)
                back[rows, 0:128] = (re * ct + im * st).astype(jnp.bfloat16)
                back[rows, 128:256] = (im * ct - re * st).astype(jnp.bfloat16)
        for c in range(owned):
            rows = slice(c * R, (c + 1) * R)
            spec[slot, rows, :] = dot(back[rows, :], w2[...])

    for i in range(9, 15):
        loads[i].wait()
    forward(pf, 0)
    all_of(hx, fs, fr).wait_recv()
    for q in range(per):
        flat[q * part : (q + 1) * part, :] = hx[:, :, q * 128 : (q + 1) * 128].astype(jnp.float32).reshape(part, 128)
    forward(flat, 1)
    ct, st = ct_ref[...], st_ref[...]
    for c in range(owned):
        rows = slice(c * R, (c + 1) * R)
        ar, ai = spec[0, rows, 0:128], spec[0, rows, 128:256]
        br, bi = spec[1, rows, 0:128], spec[1, rows, 128:256]
        back[rows, 0:128] = (ar * br - ai * bi).astype(jnp.bfloat16)
        back[rows, 128:256] = (ar * bi + ai * br).astype(jnp.bfloat16)
        u = dot(back[rows, :], w2i[...])
        ur_, ui_ = u[:, 0:128], u[:, 128:256]
        bs[0:R, c * 128 : (c + 1) * 128] = (ur_ * ct - ui_ * st).astype(jnp.bfloat16)
        bs[R : 2 * R, c * 128 : (c + 1) * 128] = (ui_ * ct + ur_ * st).astype(jnp.bfloat16)
    scale = 2.0 / (256 * R)
    for c2 in range(owned // 2):
        z = dot(f1i[...], bs[:, c2 * 256 : (c2 + 1) * 256]) * scale
        for h in range(2):
            c = 2 * c2 + h
            for q in range(per):
                flat[pl.ds(q * part + c, PEERS, stride=owned), :] = z[q * PEERS : (q + 1) * PEERS, h * 128 : h * 128 + 128]

    def cols_of(q):
        return pl.ds(q * step, step)

    wide = step // 128
    for q in range(SPANS):
        for u in range(q * wide, (q + 1) * wide):
            rows = slice(u * part, (u + 1) * part)
            gain = jnp.broadcast_to(rows_t[9][None], (PEERS, owned, 128)).reshape(part, 128)
            skipped = (flat[rows, :] + gain * pf[rows, :]).astype(jnp.bfloat16).astype(jnp.float32)
            gated = (qf[rows, :] * skipped).astype(jnp.bfloat16)
            sk[:, :, u * 128 : (u + 1) * 128] = gated.reshape(PEERS, owned, 128)
        for plane in range(2):
            each_peer(
                lambda p, b, dev: send(
                    sk.at[p, :, cols_of(q)], ret.at[plane, block, :, cols_of(q)], xsnd.at[plane, q], xrcv.at[plane, core, q], dev
                ).start(),
                plane=plane,
            )
        ret[0, block, :, q * step : (q + 1) * step] = sk[me, :, q * step : (q + 1) * step]

    lanes = lax.broadcasted_iota(jnp.int32, (128, 128), 1)
    for b in range(per):
        col = upright(ids_ref[b : b + 1, :])
        for j in range(vocab // 128):
            hot[b * 128 : (b + 1) * 128, j * 128 : (j + 1) * 128] = (col == lanes + 128 * j).astype(jnp.float32).astype(jnp.bfloat16)
    for i in range(15, 18):
        loads[i].wait()
    res[...] = dot(hot[...], rt[...])

    def slot_of(k, yy):
        return (zh if k == 0 else 1 - zh) * 4 + yy

    def direct(k, g, q, upward):
        here = buf.at[g, slot_of(k, y), cols_of(q)]
        s, r = (us, ur) if upward else (ds, dr)
        return send(here, here, s.at[k, g, q], r.at[k, g, q], {"y": up if upward else down})

    def rises(k, g, q):
        return (k + g + q) % 2 == 0

    def relay(k, g, q):
        upward = rises(k, g, q)
        here = buf.at[g, slot_of(k, down if upward else up), cols_of(q)]
        return send(here, here, ls.at[k, g, q], lr.at[k, g, q], {"y": up if upward else down})

    def returned(k, g, q, count):
        some = ret.at[k, pl.ds(16 * g, count), :, cols_of(q)]
        return send(some, some, xsnd.at[k, q], xrcv.at[k, g, q], {"y": up})

    def turn(k, g, q):
        if k == 0:

            @pl.when(core == g)
            def _():
                returned(k, g, q, 15).wait_recv()

            @pl.when(core != g)
            def _():
                returned(k, g, q, 16).wait_recv()
        else:
            returned(k, g, q, 16).wait_recv()
        for u in range(wide):
            cols = slice(q * step + u * 128, q * step + (u + 1) * 128)
            arrived = ret[k, 16 * g : 16 * (g + 1), :, cols].astype(jnp.float32).reshape(16 * owned, 128)
            buf[g, slot_of(k, y), cols, :] = jnp.transpose(arrived).astype(jnp.bfloat16)
        direct(k, g, q, True).start()
        direct(k, g, q, False).start()

    def pass_on(k, g, q):
        direct(k, g, q, rises(k, g, q)).wait_recv()
        relay(k, g, q).start()

    def finish(g, q):
        for k in range(2):
            direct(k, g, q, not rises(k, g, q)).wait_recv()
            relay(k, g, q).wait_recv()
        for u in range(wide):
            rows = slice(q * step + u * 128, q * step + (u + 1) * 128)
            left = jnp.concatenate([buf[g, j, rows, :] for j in range(TP)], axis=1)
            total = res[rows, :] + dot(left, wo[g].reshape(TP * 16 * owned, width))
            if g == 0:
                res[rows, :] = total
            else:
                o_ref[rows, :] = total.astype(jnp.bfloat16)

    chunks = [(g, q) for g in range(2) for q in range(SPANS)]
    for s in range(len(chunks) + 3):
        for k in range(2):
            if s < len(chunks):
                turn(k, *chunks[s])
            if 0 <= s - 1 < len(chunks):
                pass_on(k, *chunks[s - 1])
        if 0 <= s - 3 < len(chunks):
            finish(*chunks[s - 3])

    all_of(idall, ids_s, ids_r).wait_send()
    all_of(hx, fs, fr).wait_send()
    picks_copy.wait_send()
    for q in range(SPANS):
        for k in range(2):
            sent = sk.at[pl.ds(0, PEERS - 1 + k), :, cols_of(q)]
            send(sent, sent, xsnd.at[k, q], xrcv.at[k, 0, q], {"y": up}).wait_send()
            for g in range(2):
                direct(k, g, q, True).wait_send()
                direct(k, g, q, False).wait_send()
                relay(k, g, q).wait_send()


def local(token_ids, embed_table, norm_gain, w_in, short_taps, long_filter, skip_gain, w_out):
    vocab, width = embed_table.shape
    T = token_ids.shape[0]
    part = w_in.shape[2]
    owned = part // PEERS
    per = T // 128
    R = PEERS * per
    cols = w_out.shape[1]
    f1, ct, st, w2, w2i, f1i = tables(PEERS, per)
    bf = lambda a: jnp.asarray(a.astype(jnp.bfloat16))
    f32 = lambda a: jnp.asarray(a.astype(np.float32))
    vmem = pl.BlockSpec(memory_space=pltpu.VMEM)
    hbm = pl.BlockSpec(memory_space=pltpu.HBM)
    dma = pltpu.SemaphoreType.DMA
    B, F = jnp.bfloat16, jnp.float32
    V = pltpu.VMEM
    operands = (
        token_ids.reshape(per, 128),
        norm_gain.reshape(1, width),
        short_taps,
        skip_gain.reshape(part // 128, 128),
        f32(ct),
        f32(st),
        embed_table,
        jnp.transpose(w_in, (1, 0, 2)),
        long_filter.reshape(PEERS, owned, T),
        w_out.reshape(TP, 2, part // 2, cols),
        bf(f1),
        bf(w2),
        bf(w2i),
        bf(f1i),
    )
    return pl.pallas_call(
        block_kernel,
        out_shape=jax.ShapeDtypeStruct((T, cols), B),
        in_specs=[hbm] * 14,
        out_specs=vmem,
        scratch_shapes=[
            V((per, 128), jnp.int32),
            V((1, width), F),
            V(short_taps.shape, F),
            V((part // 128, 128), F),
            V(ct.shape, F),
            V(st.shape, F),
            V((PEERS, owned, T), B),
            V((vocab // 2, width), B),
            V((vocab // 2, width), B),
            V((width, 3 * part), B),
            V((vocab, cols), B),
            V((2, vocab // 256, 4 * owned, 128), B),
            V((vocab // 128, 4 * owned, 128), B),
            V((T, vocab), B),
            V((2, TP, part // 2, cols), B),
            V(f1.shape, B),
            V(w2.shape, B),
            V(w2i.shape, B),
            V(f1i.shape, B),
            V((per // 2, 128), jnp.int32),
            V((PEERS, per // 2, 128), jnp.int32),
            V((128, 128), F),
            V((10, owned, 128), F),
            V((PEERS, owned, T), B),
            V((per * part, 128), F),
            V((per * part, 128), F),
            V((T, cols), F),
            V((per * part, 128), F),
            V((R, owned * 128), B),
            V((2, owned * R, 256), F),
            V((owned * R, 256), B),
            V((2 * R, owned * 128), B),
            V((PEERS, owned, T), B),
            V((2, PEERS, owned, T), B),
            V((2, TP, T, part // 2), B),
            dma((18,)),
            dma,
            dma,
            dma,
            dma,
            dma,
            dma,
        ]
        + [dma((2, SPANS))] + [dma((2, 2, SPANS))] * 7,
        compiler_params=pltpu.CompilerParams(collective_id=0, has_side_effects=True, vmem_limit_bytes=48 * 2**20),
        name="block",
    )(*(pltpu.with_memory_space_constraint(a, pltpu.HBM) for a in operands))


def solution(mesh):
    finer = Mesh(mesh.devices.reshape(4, 4, 2, 2, 4), ("x", "zl", "core", "zh", "y"))
    tp = ("zh", "y")
    in_specs = (
        P(CTX),
        P(),
        P(),
        P(None, None, tp),
        P(None, None, tp),
        P(tp, CTX),
        P(tp),
        P(None, tp),
    )
    return jax.shard_map(local, mesh=finer, in_specs=in_specs, out_specs=P(CTX, tp), check_vma=False)
```

```python
import functools
import math

import jax
import jax.numpy as jnp
import numpy as np
from jax import lax
from jax.experimental import pallas as pl
from jax.experimental.pallas import tpu as pltpu
from jax.sharding import Mesh
from jax.sharding import PartitionSpec as P

CTX = ("x", "zl", "core")
MESH = pl.DeviceIdType.MESH
PEERS = 32
TP = 8
norm_eps = 1e-06


@functools.lru_cache(maxsize=None)
def tables(peers, per):
    R = peers * per
    N = 256 * R
    order = (np.arange(per)[:, None] + per * np.arange(peers)[None, :]).reshape(-1)
    k1 = np.arange(R) + 0.5
    a1 = 2 * np.pi * np.outer(k1, order) / (2 * R)
    f1 = np.concatenate([np.cos(a1), -np.sin(a1)], 0)
    at = 2 * np.pi * np.outer(k1, np.arange(128)) / N
    a2 = 2 * np.pi * (np.outer(np.arange(128), np.arange(128)) % 128) / 128
    c, s = np.cos(a2), np.sin(a2)
    w2 = np.block([[c, -s], [s, c]])
    w2i = np.block([[c, s], [-s, c]])
    f1i = np.concatenate([np.cos(a1.T), -np.sin(a1.T)], 1)
    return f1, np.cos(at), np.sin(at), w2, w2i, f1i


def peer_of(p):
    return {"x": p // 8, "zl": lax.rem(p // 2, 4), "core": lax.rem(p, 2)}


def ctx_index():
    return lax.axis_index("x") * 8 + lax.axis_index("zl") * 2 + lax.axis_index("core")


def dot(a, b):
    return jnp.dot(a, b, preferred_element_type=jnp.float32)


def send(src, dst, s, r, dev):
    return pltpu.make_async_remote_copy(
        src_ref=src, dst_ref=dst, send_sem=s, recv_sem=r, device_id=dev, device_id_type=MESH
    )


CHUNKS = 6
AHEAD = 3
CROSS = (2, 3)
UNROLL = 3


def normalize(tv, gain_ref, nv, first, last):
    width = tv.shape[1]

    @pl.loop(first, last)
    def _(r):
        rows = pl.ds(pl.multiple_of(r * 32, 32), 32)
        acc = jnp.zeros((32, 128), jnp.float32)
        for j in range(width // 128):
            x = tv[rows, j * 128 : (j + 1) * 128].astype(jnp.float32)
            acc += x * x
        scale = lax.rsqrt(jnp.sum(acc, axis=1, keepdims=True) * (1.0 / width) + norm_eps)
        for j in range(width // 128):
            cols = slice(j * 128, (j + 1) * 128)
            x = tv[rows, cols].astype(jnp.float32)
            nv[rows, cols] = (x * scale * gain_ref[:, cols]).astype(jnp.bfloat16)


def upright(row):
    return jnp.transpose(jnp.broadcast_to(row, (128, 128)))


def low_high(a, b):
    axis = a.ndim - 2
    first = lax.broadcasted_iota(jnp.int32, a.shape, axis) < 4
    return jnp.where(first, a, pltpu.roll(b, 4, axis)), jnp.where(first, pltpu.roll(a, 4, axis), b)


def block_kernel(
    ids_hbm, gain_hbm, taps_hbm, skip_hbm, ct_hbm, st_hbm, table_hbm, w3_hbm, filt_hbm, wo_hbm, f1_hbm, w2_hbm, w2i_hbm, f1i_hbm,
    o_ref,
    ids_ref, gain_ref, taps_ref, skip_ref, ct_ref, st_ref, fv, fsend, tv, nv, wv, rt, halves, picks, hot, wo, f1, w2, w2i, f1i,
    idpair, idall, column, rows_t, hx, pf, qf, res, flat, xs, spec, back, bs, sk, ret, buf,
    ld, ids_s, ids_r, fs, fr, pk_s, pk_r, xsnd, xrcv, zs, us, ur, ds, dr, ls, lr,
):
    x, zl, core = lax.axis_index("x"), lax.axis_index("zl"), lax.axis_index("core")
    me = ctx_index()
    zh, y = lax.axis_index("zh"), lax.axis_index("y")
    own = zh * 4 + y
    up, down = lax.rem(y + 1, 4), lax.rem(y + 3, 4)
    mine = tv.shape[0]
    vocab = 2 * mine
    owned = fv.shape[1]
    few = owned // 2
    part = PEERS * owned
    T = res.shape[0]
    width = o_ref.shape[1]
    per = T // 128
    spans = per // 2
    R = PEERS * per
    half = me // 16
    pair = pl.multiple_of(lax.rem(me, 16) // 2 * owned, owned)

    def owned_rows(ref, base):
        return low_high(
            ref[pl.ds(pl.multiple_of(base + pair, owned), owned), :], ref[pl.ds(pl.multiple_of(base + 64 + pair, owned), owned), :]
        )

    def each_peer(planes, fn):
        planes = range(planes) if isinstance(planes, int) else planes

        def chip(t, skip_self):
            px, pz = lax.rem(x + t // 4, 4), lax.rem(zl + lax.rem(t, 4), 4)
            for dc in range(2):
                pc = lax.rem(core + dc, 2)
                p = px * 8 + pz * 2 + pc
                for k in planes:
                    if not (skip_self and dc == 0 and k == 0):
                        dev = {"x": px, "zl": pz, "core": pc}
                        if k == 1:
                            dev["zh"] = 1 - zh
                        fn(p, k, dev)

        def go(t, carry):
            chip(t, False)
            return carry

        lax.fori_loop(1, 16, go, 0, unroll=UNROLL)
        chip(0, True)

    bar = pltpu.get_barrier_semaphore()

    def greet(dev):
        pl.semaphore_signal(bar, inc=1, device_id=dev, device_id_type=MESH)

    each_peer(2, lambda p, k, dev: greet(dev))
    greet({"y": up})
    greet({"y": down})

    pairs = (
        [
            (ids_hbm, ids_ref),
            (filt_hbm, fv),
            (table_hbm.at[pl.ds(pl.multiple_of(core * mine, mine), mine)], tv),
            (gain_hbm, gain_ref),
            (taps_hbm, taps_ref),
            (skip_hbm, skip_ref),
        ]
        + [(w3_hbm.at[s, :, pl.ds(pl.multiple_of(half * 128, 128), 128)], wv.at[:, pl.ds(s * 128, 128)]) for s in range(3)]
        + [
            (ct_hbm, ct_ref),
            (st_hbm, st_ref),
            (f1_hbm, f1),
            (w2_hbm, w2),
            (w2i_hbm, w2i),
            (f1i_hbm, f1i),
            (table_hbm.at[:, pl.ds(pl.multiple_of(own * width, width), width)], rt),
        ]
        + [(wo_hbm.at[:, a, h], wo.at[h, :, pl.ds(64 * a, 64)]) for a in range(2) for h in range(2)]
    )
    loads = [pltpu.make_async_copy(a, b, ld.at[i]) for i, (a, b) in enumerate(pairs)]
    for c in loads:
        c.start()
    for i in range(2):
        loads[i].wait()
    idpair[...] = ids_ref[0:spans, :] + ids_ref[spans:per, :] * 65536
    for h in range(2):
        for a in range(2):
            t0 = a * 16 + h * 8
            tiles = fv[t0 : t0 + 8].astype(jnp.float32)
            even, odd = low_high(tiles[:, :, : T // 2], tiles[:, :, T // 2 :])
            fsend[h, a * 16 : (a + 1) * 16] = jnp.stack([even, odd], axis=1).reshape(16, owned, T // 2).astype(jnp.bfloat16)
    pl.semaphore_wait(bar, 2 * PEERS + 1)

    each_peer(1, lambda p, k, dev: send(idpair, idall.at[me], ids_s, ids_r, dev).start())
    for h in range(2):
        each_peer(1, lambda p, k, dev: send(fsend.at[h, p], hx.at[h, me], fs.at[h], fr.at[h], dev).start())

    def all_of(ref, s, r):
        most = ref.at[pl.ds(0, PEERS - 1)]
        return send(most, most, s, r, {"y": up})

    idall[me] = idpair[...]
    for h in range(2):
        hx[h, me] = fsend[h, me]

    for i in range(2, 4):
        loads[i].wait()
    normalize(tv, gain_ref, nv, 0, mine // 32)
    for s in range(3):
        loads[6 + s].wait()
    for n0, n1 in ((0, 256), (256, 384)):
        projected = dot(nv[...], wv[:, n0:n1]).astype(jnp.bfloat16).astype(jnp.float32)
        for n in range(n0, n1, 128):
            for v in range(mine // 128):
                row = (n // 128 * 2 + v) * 128
                flat[row : row + 128, :] = jnp.transpose(projected[v * 128 : (v + 1) * 128, n - n0 : n - n0 + 128])
    for v in range(mine // 128):
        found = [owned_rows(flat, (s * 2 + v) * 128) for s in range(3)]
        for c in range(2):
            rows = [f[c] for f in found] + [jnp.zeros((owned, 128), jnp.float32)]
            halves[c, v] = jnp.concatenate(rows, axis=0).astype(jnp.bfloat16)
    groups = vocab // 128
    picks_copy = send(halves.at[1 - core], picks.at[pl.ds(2 * core, 2)], pk_s, pk_r, {"core": 1 - core})
    picks_copy.start()
    picks[pl.ds(2 * core, 2)] = halves[core]

    for i in range(4, 6):
        loads[i].wait()

    def own_column(row_a, row_b, to):
        column[...] = upright(jnp.where(half == 0, row_a, row_b))
        low, high = owned_rows(column, 0)
        rows_t[to] = jnp.where(core == 0, low, high)

    for r in range(3):
        for s in range(3):
            own_column(taps_ref[r, s : s + 1, 0:128], taps_ref[r, s : s + 1, 128:256], r * 3 + s)
    own_column(skip_ref[0:1, :], skip_ref[1:2, :], 9)

    all_of(idall, ids_s, ids_r).wait_recv()
    picks_copy.wait_recv()
    table_rows = picks[...].reshape(groups * 4 * owned, 128)
    lane = lax.broadcasted_iota(jnp.int32, (owned, 128), 1)
    token = lax.broadcasted_iota(jnp.int32, (128, 128), 0)

    def positions(i, carry):
        products, queries = [], []
        for q2 in range(per // 2):
            both = [idall[i, q % spans : q % spans + 1, :] for q in (2 * q2, 2 * q2 + 1)]
            both = [ids & 65535 if 2 * q2 + h < spans else ids >> 16 for h, ids in enumerate(both)]
            hits = [(jnp.broadcast_to(ids & 127, (128, 128)) == token).astype(jnp.float32).astype(jnp.bfloat16) for ids in both]
            chosen = dot(table_rows, jnp.concatenate(hits, axis=1))
            for h in range(2):
                group = jnp.broadcast_to(both[h] >> 7, (owned, 128))
                short, later = [], []
                for s in range(3):
                    of = [
                        chosen[(v * 4 + s) * owned : (v * 4 + s + 1) * owned, h * 128 : (h + 1) * 128] for v in range(groups)
                    ]
                    now = of[0]
                    for v in range(1, groups):
                        now = jnp.where(group == v, of[v], now)
                    by1, by2 = pltpu.roll(now, 1, 1), pltpu.roll(now, 2, 1)
                    before1, before2 = carry[s]
                    one = jnp.where(lane < 1, before1, by1)
                    two = jnp.where(lane < 2, before2, by2)
                    short.append(
                        (rows_t[s] * now + rows_t[3 + s] * one + rows_t[6 + s] * two).astype(jnp.bfloat16).astype(jnp.float32)
                    )
                    later.append((by1, by2))
                carry = tuple(later)
                products.append((short[1] * short[2]).astype(jnp.bfloat16).astype(jnp.float32))
                queries.append(short[0])
        for u in range(spans):
            rows = pl.ds(pl.multiple_of(u * part + i * owned, owned), owned)
            pf[0, rows, :], pf[1, rows, :] = low_high(products[u], products[u + spans])
            qf[0, rows, :], qf[1, rows, :] = low_high(queries[u], queries[u + spans])
        return carry

    nothing = jnp.zeros((owned, 128), jnp.float32)
    lax.fori_loop(0, PEERS, positions, ((nothing, nothing),) * 3, unroll=4)

    def lines(c, q):
        return pl.ds(q % spans * part + c + few * (q // spans), PEERS, stride=owned)

    def forward(src, slot):
        for c in range(few):
            for q in range(per):
                xs[q * PEERS : (q + 1) * PEERS, c * 128 : (c + 1) * 128] = src[lines(c, q), :].astype(jnp.bfloat16)
        ct, st = ct_ref[...], st_ref[...]
        for c2 in range(few // 2):
            first = dot(f1[...], xs[:, c2 * 256 : (c2 + 1) * 256])
            for h in range(2):
                c = 2 * c2 + h
                re = first[:R, h * 128 : h * 128 + 128]
                im = first[R:, h * 128 : h * 128 + 128]
                rows = slice(c * R, (c + 1) * R)
                back[rows, 0:128] = (re * ct + im * st).astype(jnp.bfloat16)
                back[rows, 128:256] = (im * ct - re * st).astype(jnp.bfloat16)
        for c in range(few):
            rows = slice(c * R, (c + 1) * R)
            spec[slot, rows, :] = dot(back[rows, :], w2[...])

    def convolve(half_index, slot):
        for u in range(spans):
            flat[u * part : (u + 1) * part, :] = (
                hx[half_index, :, :, u * 128 : (u + 1) * 128].astype(jnp.float32).reshape(part, 128)
            )
        forward(flat, 2)
        ct, st = ct_ref[...], st_ref[...]
        for c in range(few):
            rows = slice(c * R, (c + 1) * R)
            ar, ai = spec[slot, rows, 0:128], spec[slot, rows, 128:256]
            br, bi = spec[2, rows, 0:128], spec[2, rows, 128:256]
            back[rows, 0:128] = (ar * br - ai * bi).astype(jnp.bfloat16)
            back[rows, 128:256] = (ar * bi + ai * br).astype(jnp.bfloat16)
            u = dot(back[rows, :], w2i[...])
            ur_, ui_ = u[:, 0:128], u[:, 128:256]
            bs[0:R, c * 128 : (c + 1) * 128] = (ur_ * ct - ui_ * st).astype(jnp.bfloat16)
            bs[R : 2 * R, c * 128 : (c + 1) * 128] = (ui_ * ct + ur_ * st).astype(jnp.bfloat16)
        scale = 2.0 / (256 * R)
        for c2 in range(few // 2):
            z = dot(f1i[...], bs[:, c2 * 256 : (c2 + 1) * 256]) * scale
            for h in range(2):
                for q in range(per):
                    flat[lines(2 * c2 + h, q), :] = z[q * PEERS : (q + 1) * PEERS, h * 128 : h * 128 + 128]
        gain = low_high(rows_t[9], rows_t[9])[half_index]
        gain = jnp.broadcast_to(gain[None], (PEERS, owned, 128)).reshape(part, 128)
        for u in range(spans):
            rows = slice(u * part, (u + 1) * part)
            skipped = (flat[rows, :] + gain * pf[half_index, rows, :]).astype(jnp.bfloat16).astype(jnp.float32)
            gated = (qf[half_index, rows, :] * skipped).astype(jnp.bfloat16)
            sk[half_index, :, :, u * 128 : (u + 1) * 128] = gated.reshape(PEERS, owned, 128)
        ret[half_index, 0, me] = sk[half_index, me]

    chunks = [(h, u) for h in range(2) for u in range(spans)]

    def emit(c):
        h, u = chunks[c]
        cols = pl.ds(u * 128, 128)
        for plane in range(2):
            each_peer(
                (plane,),
                lambda p, k, dev: send(sk.at[h, p, :, cols], ret.at[h, k, me, :, cols], xsnd.at[k, c], xrcv.at[k, c], dev).start(),
            )

    for i in range(9, 16):
        loads[i].wait()
    forward(pf.at[0], 0)
    all_of(hx.at[0], fs.at[0], fr.at[0]).wait_recv()
    convolve(0, 0)
    for c in range(spans):
        emit(c)
    forward(pf.at[1], 1)
    lanes = lax.broadcasted_iota(jnp.int32, (128, 128), 1)
    for b in range(per):
        col = upright(ids_ref[b : b + 1, :])
        for j in range(vocab // 128):
            hot[b * 128 : (b + 1) * 128, j * 128 : (j + 1) * 128] = (col == lanes + 128 * j).astype(jnp.float32).astype(jnp.bfloat16)
    res[...] = dot(hot[...], rt[...])
    all_of(hx.at[1], fs.at[1], fr.at[1]).wait_recv()
    convolve(1, 1)

    def slot_of(k, yy):
        return (zh if k == 0 else 1 - zh) * 4 + yy

    def piece(c, slot):
        h, u = chunks[c]
        return buf.at[h, slot, u]

    def direct(k, c, upward):
        here = piece(c, slot_of(k, y))
        s, r = (us, ur) if upward else (ds, dr)
        return send(here, here, s.at[k, c], r.at[k, c], {"y": up if upward else down})

    def relay(k, c):
        if k == 1 and c in CROSS:
            here = piece(c, slot_of(0, lax.rem(y + 2, 4)))
            return send(here, here, ls.at[k, c], lr.at[k, c], {"zh": 1 - zh})
        upward = (c + k) % 2 == 0
        here = piece(c, slot_of(k, down if upward else up))
        return send(here, here, ls.at[k, c], lr.at[k, c], {"y": up if upward else down})

    def returned(k, c):
        h, u = chunks[c]
        most = ret.at[h, k, pl.ds(0, PEERS - 1 + k), :, pl.ds(u * 128, 128)]
        return send(most, most, xsnd.at[k, c], xrcv.at[k, c], {"y": up})

    def turn(k, c):
        h, u = chunks[c]
        returned(k, c).wait_recv()
        tiles = ret[h, k, :, :, u * 128 : (u + 1) * 128].astype(jnp.float32).reshape(PEERS // 2, 2, owned, 128)
        for b, rows in enumerate(low_high(tiles[:, 0], tiles[:, 1])):
            buf[h, slot_of(k, y), u, b * 128 : (b + 1) * 128, :] = jnp.transpose(rows.reshape(128, 128)).astype(jnp.bfloat16)
        direct(k, c, True).start()
        direct(k, c, False).start()

    def pass_on(k, c):
        if k == 1 and c in CROSS:
            relay(0, c).wait_recv()
        else:
            direct(k, c, (c + k) % 2 == 0).wait_recv()
        relay(k, c).start()

    def finish(c):
        h, u = chunks[c]
        for k in range(2):
            direct(k, c, (c + k) % 2 == 1).wait_recv()
            if k == 1 and c in CROSS:
                direct(k, c, (c + k) % 2 == 0).wait_recv()
            if not (k == 0 and c in CROSS):
                relay(k, c).wait_recv()
        for b in range(2):
            q = u + b * spans
            rows = slice(q * 128, (q + 1) * 128)
            left = jnp.concatenate([buf[h, j, u, b * 128 : (b + 1) * 128, :] for j in range(TP)], axis=1)
            total = res[rows, :] + dot(left, wo[h].reshape(TP * 128, width))
            if h == 0:
                res[rows, :] = total
            else:
                o_ref[rows, :] = total.astype(jnp.bfloat16)

    for i in range(16, 20):
        loads[i].wait()
    for s in range(CHUNKS + 3):
        for k in range(2):
            if s < CHUNKS:
                turn(k, s)
            if 0 <= s - 1 < CHUNKS and not (k == 1 and s - 1 in CROSS):
                pass_on(k, s - 1)
        if s + AHEAD < CHUNKS:
            emit(s + AHEAD)
        if s - 2 in CROSS:
            pass_on(1, s - 2)
        if 0 <= s - 3 < CHUNKS:
            finish(s - 3)

    all_of(idall, ids_s, ids_r).wait_send()
    picks_copy.wait_send()
    for h in range(2):
        all_of(hx.at[h], fs.at[h], fr.at[h]).wait_send()
    for c in range(CHUNKS):
        for k in range(2):
            returned(k, c).wait_send()
            direct(k, c, True).wait_send()
            direct(k, c, False).wait_send()
            relay(k, c).wait_send()


def local(token_ids, embed_table, norm_gain, w_in, short_taps, long_filter, skip_gain, w_out):
    vocab, width = embed_table.shape
    T = token_ids.shape[0]
    part = w_in.shape[2]
    owned = part // PEERS
    per = T // 128
    R = PEERS * per
    cols = w_out.shape[1]
    f1, ct, st, w2, w2i, f1i = tables(PEERS, per)
    bf = lambda a: jnp.asarray(a.astype(jnp.bfloat16))
    f32 = lambda a: jnp.asarray(a.astype(np.float32))
    vmem = pl.BlockSpec(memory_space=pltpu.VMEM)
    hbm = pl.BlockSpec(memory_space=pltpu.HBM)
    dma = pltpu.SemaphoreType.DMA
    B, F = jnp.bfloat16, jnp.float32
    V = pltpu.VMEM
    operands = (
        token_ids.reshape(per, 128),
        norm_gain.reshape(1, width),
        short_taps,
        skip_gain.reshape(part // 128, 128),
        f32(ct),
        f32(st),
        embed_table,
        jnp.transpose(w_in, (1, 0, 2)),
        long_filter.reshape(PEERS, owned, T),
        w_out.reshape(TP, 2, 2, part // 4, cols),
        bf(f1),
        bf(w2),
        bf(w2i),
        bf(f1i),
    )
    return pl.pallas_call(
        block_kernel,
        out_shape=jax.ShapeDtypeStruct((T, cols), B),
        in_specs=[hbm] * 14,
        out_specs=vmem,
        scratch_shapes=[
            V((per, 128), jnp.int32),
            V((1, width), F),
            V(short_taps.shape, F),
            V((part // 128, 128), F),
            V(ct.shape, F),
            V(st.shape, F),
            V((PEERS, owned, T), B),
            V((2, PEERS, owned, T // 2), B),
            V((vocab // 2, width), B),
            V((vocab // 2, width), B),
            V((width, 384), B),
            V((vocab, cols), B),
            V((2, vocab // 256, 4 * owned, 128), B),
            V((vocab // 128, 4 * owned, 128), B),
            V((T, vocab), B),
            V((2, TP, part // 2, cols), B),
            V(f1.shape, B),
            V(w2.shape, B),
            V(w2i.shape, B),
            V(f1i.shape, B),
            V((per // 2, 128), jnp.int32),
            V((PEERS, per // 2, 128), jnp.int32),
            V((128, 128), F),
            V((10, owned, 128), F),
            V((2, PEERS, owned, T // 2), B),
            V((2, per // 2 * part, 128), F),
            V((2, per // 2 * part, 128), F),
            V((T, cols), F),
            V((per // 2 * part, 128), F),
            V((R, owned // 2 * 128), B),
            V((3, owned // 2 * R, 256), F),
            V((owned // 2 * R, 256), B),
            V((2 * R, owned // 2 * 128), B),
            V((2, PEERS, owned, T // 2), B),
            V((2, 2, PEERS, owned, T // 2), B),
            V((2, TP, per // 2, 256, part // 2), B),
            dma((20,)),
            dma,
            dma,
            dma((2,)),
            dma((2,)),
            dma,
            dma,
        ]
        + [dma((2, CHUNKS))] * 9,
        compiler_params=pltpu.CompilerParams(collective_id=0, has_side_effects=True, vmem_limit_bytes=48 * 2**20),
        name="block",
    )(*(pltpu.with_memory_space_constraint(a, pltpu.HBM) for a in operands))


def solution(mesh):
    finer = Mesh(mesh.devices.reshape(4, 4, 2, 2, 4), ("x", "zl", "core", "zh", "y"))
    tp = ("zh", "y")
    in_specs = (
        P(CTX),
        P(),
        P(),
        P(None, None, tp),
        P(None, None, tp),
        P(tp, CTX),
        P(tp),
        P(None, tp),
    )
    return jax.shard_map(local, mesh=finer, in_specs=in_specs, out_specs=P(CTX, tp), check_vma=False)
```

```python
import functools
import math

import jax
import jax.numpy as jnp
import numpy as np
from jax import lax
from jax.experimental import pallas as pl
from jax.experimental.pallas import tpu as pltpu
from jax.sharding import Mesh
from jax.sharding import PartitionSpec as P

CTX = ("x", "zl", "core")
MESH = pl.DeviceIdType.MESH
PEERS = 32
TP = 8
norm_eps = 1e-06


@functools.lru_cache(maxsize=None)
def tables(peers, per):
    R = peers * per
    N = 256 * R
    order = (np.arange(per)[:, None] + per * np.arange(peers)[None, :]).reshape(-1)
    k1 = np.arange(R) + 0.5
    a1 = 2 * np.pi * np.outer(k1, order) / (2 * R)
    f1 = np.concatenate([np.cos(a1), -np.sin(a1)], 0)
    at = 2 * np.pi * np.outer(k1, np.arange(128)) / N
    a2 = 2 * np.pi * (np.outer(np.arange(128), np.arange(128)) % 128) / 128
    c, s = np.cos(a2), np.sin(a2)
    w2 = np.block([[c, -s], [s, c]])
    w2i = np.block([[c, s], [-s, c]])
    f1i = np.concatenate([np.cos(a1.T), -np.sin(a1.T)], 1)
    return f1, np.cos(at), np.sin(at), w2, w2i, f1i


def peer_of(p):
    return {"x": p // 8, "zl": lax.rem(p // 2, 4), "core": lax.rem(p, 2)}


def ctx_index():
    return lax.axis_index("x") * 8 + lax.axis_index("zl") * 2 + lax.axis_index("core")


def dot(a, b):
    return jnp.dot(a, b, preferred_element_type=jnp.float32)


def send(src, dst, s, r, dev):
    return pltpu.make_async_remote_copy(
        src_ref=src, dst_ref=dst, send_sem=s, recv_sem=r, device_id=dev, device_id_type=MESH
    )


CHUNKS = 6
AHEAD = 3
CROSS = (2, 3)
UNROLL = 3


def normalize(tv, gain_ref, nv, first, last):
    width = tv.shape[1]

    @pl.loop(first, last, unroll=2)
    def _(r):
        rows = pl.ds(pl.multiple_of(r * 32, 32), 32)
        acc = jnp.zeros((32, 128), jnp.float32)
        for j in range(width // 128):
            x = tv[rows, j * 128 : (j + 1) * 128].astype(jnp.float32)
            acc += x * x
        scale = lax.rsqrt(jnp.sum(acc, axis=1, keepdims=True) * (1.0 / width) + norm_eps)
        for j in range(width // 128):
            cols = slice(j * 128, (j + 1) * 128)
            x = tv[rows, cols].astype(jnp.float32)
            nv[rows, cols] = (x * scale * gain_ref[:, cols]).astype(jnp.bfloat16)


def upright(row):
    return jnp.transpose(jnp.broadcast_to(row, (128, 128)))


def low_high(a, b):
    axis = a.ndim - 2
    first = lax.broadcasted_iota(jnp.int32, a.shape, axis) < 4
    return jnp.where(first, a, pltpu.roll(b, 4, axis)), jnp.where(first, pltpu.roll(a, 4, axis), b)


def block_kernel(
    ids_hbm, gain_hbm, taps_hbm, skip_hbm, ct_hbm, st_hbm, table_hbm, w3_hbm, filt_hbm, wo_hbm, f1_hbm, w2_hbm, w2i_hbm, f1i_hbm,
    o_ref,
    ids_ref, gain_ref, taps_ref, skip_ref, ct_ref, st_ref, fv, fsend, tv, nv, wv, rt, halves, picks, hot, wo, f1, w2, w2i, f1i,
    idpair, idall, column, rows_t, hx, pf, qf, res, flat, xs, spec, back, bs, sk, ret, buf,
    ld, ids_s, ids_r, fs, fr, pk_s, pk_r, xsnd, xrcv, us, ur, ds, dr, ls, lr,
):
    x, zl, core = lax.axis_index("x"), lax.axis_index("zl"), lax.axis_index("core")
    me = ctx_index()
    zh, y = lax.axis_index("zh"), lax.axis_index("y")
    own = zh * 4 + y
    up, down = lax.rem(y + 1, 4), lax.rem(y + 3, 4)
    mine = tv.shape[0]
    vocab = 2 * mine
    owned = fv.shape[1]
    few = owned // 2
    part = PEERS * owned
    T = res.shape[0]
    width = o_ref.shape[1]
    per = T // 128
    spans = per // 2
    R = PEERS * per
    half = me // 16
    pair = pl.multiple_of(lax.rem(me, 16) // 2 * owned, owned)

    def owned_rows(ref, base):
        return low_high(
            ref[pl.ds(pl.multiple_of(base + pair, owned), owned), :], ref[pl.ds(pl.multiple_of(base + 64 + pair, owned), owned), :]
        )

    def each_peer(planes, fn):
        planes = range(planes) if isinstance(planes, int) else planes

        def chip(t, skip_self):
            px, pz = lax.rem(x + t // 4, 4), lax.rem(zl + lax.rem(t, 4), 4)
            for dc in range(2):
                pc = lax.rem(core + dc, 2)
                p = px * 8 + pz * 2 + pc
                for k in planes:
                    if not (skip_self and dc == 0 and k == 0):
                        dev = {"x": px, "zl": pz, "core": pc}
                        if k == 1:
                            dev["zh"] = 1 - zh
                        fn(p, k, dev)

        def go(t, carry):
            chip(t, False)
            return carry

        lax.fori_loop(1, 16, go, 0, unroll=UNROLL)
        chip(0, True)

    bar = pltpu.get_barrier_semaphore()

    def greet(dev):
        pl.semaphore_signal(bar, inc=1, device_id=dev, device_id_type=MESH)

    each_peer(2, lambda p, k, dev: greet(dev))
    greet({"y": up})
    greet({"y": down})

    pairs = (
        [
            (ids_hbm, ids_ref),
            (filt_hbm, fv),
            (table_hbm.at[pl.ds(pl.multiple_of(core * mine, mine), mine)], tv),
            (gain_hbm, gain_ref),
            (taps_hbm, taps_ref),
            (skip_hbm, skip_ref),
        ]
        + [(w3_hbm.at[s, :, pl.ds(pl.multiple_of(half * 128, 128), 128)], wv.at[:, pl.ds(s * 128, 128)]) for s in range(3)]
        + [
            (ct_hbm, ct_ref),
            (st_hbm, st_ref),
            (f1_hbm, f1),
            (w2_hbm, w2),
            (w2i_hbm, w2i),
            (f1i_hbm, f1i),
            (table_hbm.at[:, pl.ds(pl.multiple_of(own * width, width), width)], rt),
        ]
        + [(wo_hbm.at[:, a, h], wo.at[h, :, pl.ds(64 * a, 64)]) for a in range(2) for h in range(2)]
    )
    loads = [pltpu.make_async_copy(a, b, ld.at[i]) for i, (a, b) in enumerate(pairs)]
    for c in loads:
        c.start()
    for i in range(2):
        loads[i].wait()
    idpair[...] = ids_ref[0:spans, :] + ids_ref[spans:per, :] * 65536
    for h in range(2):
        for a in range(2):
            t0 = a * 16 + h * 8
            tiles = fv[t0 : t0 + 8].astype(jnp.float32)
            even, odd = low_high(tiles[:, :, : T // 2], tiles[:, :, T // 2 :])
            fsend[h, a * 16 : (a + 1) * 16] = jnp.stack([even, odd], axis=1).reshape(16, owned, T // 2).astype(jnp.bfloat16)
    pl.semaphore_wait(bar, 2 * PEERS + 1)

    each_peer(1, lambda p, k, dev: send(idpair, idall.at[me], ids_s, ids_r, dev).start())

    def send_filter(h):
        each_peer(1, lambda p, k, dev: send(fsend.at[h, p], hx.at[h, me], fs.at[h], fr.at[h], dev).start())

    send_filter(0)

    def all_of(ref, s, r):
        most = ref.at[pl.ds(0, PEERS - 1)]
        return send(most, most, s, r, {"y": up})

    idall[me] = idpair[...]
    for h in range(2):
        hx[h, me] = fsend[h, me]

    for i in range(2, 4):
        loads[i].wait()
    normalize(tv, gain_ref, nv, 0, mine // 32)
    for s in range(3):
        loads[6 + s].wait()
    for n0, n1 in ((0, 256), (256, 384)):
        projected = dot(nv[...], wv[:, n0:n1]).astype(jnp.bfloat16).astype(jnp.float32)
        for n in range(n0, n1, 128):
            for v in range(mine // 128):
                row = (n // 128 * 2 + v) * 128
                flat[row : row + 128, :] = jnp.transpose(projected[v * 128 : (v + 1) * 128, n - n0 : n - n0 + 128])
    for v in range(mine // 128):
        found = [owned_rows(flat, (s * 2 + v) * 128) for s in range(3)]
        for c in range(2):
            rows = [f[c] for f in found] + [jnp.zeros((owned, 128), jnp.float32)]
            halves[c, v] = jnp.concatenate(rows, axis=0).astype(jnp.bfloat16)
    groups = vocab // 128
    picks_copy = send(halves.at[1 - core], picks.at[pl.ds(2 * core, 2)], pk_s, pk_r, {"core": 1 - core})
    picks_copy.start()
    picks[pl.ds(2 * core, 2)] = halves[core]

    for i in range(4, 6):
        loads[i].wait()

    def own_column(row_a, row_b, to):
        column[...] = upright(jnp.where(half == 0, row_a, row_b))
        low, high = owned_rows(column, 0)
        rows_t[to] = jnp.where(core == 0, low, high)

    for r in range(3):
        for s in range(3):
            own_column(taps_ref[r, s : s + 1, 0:128], taps_ref[r, s : s + 1, 128:256], r * 3 + s)
    own_column(skip_ref[0:1, :], skip_ref[1:2, :], 9)

    all_of(idall, ids_s, ids_r).wait_recv()
    send_filter(1)
    picks_copy.wait_recv()
    table_rows = picks[...].astype(jnp.float32)[:, : 3 * owned, :].reshape(groups * 3 * owned, 128).astype(jnp.bfloat16)
    lane = lax.broadcasted_iota(jnp.int32, (owned, 128), 1)
    token = lax.broadcasted_iota(jnp.int32, (128, 128), 0)

    def positions(i, carry):
        products, queries = [], []
        for q2 in range(per // 2):
            both = [idall[i, q % spans : q % spans + 1, :] for q in (2 * q2, 2 * q2 + 1)]
            both = [ids & 65535 if 2 * q2 + h < spans else ids >> 16 for h, ids in enumerate(both)]
            hits = [(jnp.broadcast_to(ids & 127, (128, 128)) == token).astype(jnp.float32).astype(jnp.bfloat16) for ids in both]
            chosen = dot(table_rows, jnp.concatenate(hits, axis=1))
            for h in range(2):
                group = jnp.broadcast_to(both[h] >> 7, (owned, 128))
                short, later = [], []
                for s in range(3):
                    of = [
                        chosen[(v * 3 + s) * owned : (v * 3 + s + 1) * owned, h * 128 : (h + 1) * 128] for v in range(groups)
                    ]
                    now = of[0]
                    for v in range(1, groups):
                        now = jnp.where(group == v, of[v], now)
                    by1, by2 = pltpu.roll(now, 1, 1), pltpu.roll(now, 2, 1)
                    before1, before2 = carry[s]
                    one = jnp.where(lane < 1, before1, by1)
                    two = jnp.where(lane < 2, before2, by2)
                    short.append(
                        (rows_t[s] * now + rows_t[3 + s] * one + rows_t[6 + s] * two).astype(jnp.bfloat16).astype(jnp.float32)
                    )
                    later.append((by1, by2))
                carry = tuple(later)
                products.append((short[1] * short[2]).astype(jnp.bfloat16).astype(jnp.float32))
                queries.append(short[0])
        for u in range(spans):
            rows = pl.ds(pl.multiple_of(u * part + i * owned, owned), owned)
            pf[0, rows, :], pf[1, rows, :] = low_high(products[u], products[u + spans])
            qf[0, rows, :], qf[1, rows, :] = low_high(queries[u], queries[u + spans])
        return carry

    nothing = jnp.zeros((owned, 128), jnp.float32)
    lax.fori_loop(0, PEERS, positions, ((nothing, nothing),) * 3, unroll=8)

    def lines(c, q):
        return pl.ds(q % spans * part + c + few * (q // spans), PEERS, stride=owned)

    def forward(src, slot):
        for c in range(few):
            for q in range(per):
                xs[q * PEERS : (q + 1) * PEERS, c * 128 : (c + 1) * 128] = src[lines(c, q), :].astype(jnp.bfloat16)
        ct, st = ct_ref[...], st_ref[...]
        for c2 in range(few // 2):
            first = dot(f1[...], xs[:, c2 * 256 : (c2 + 1) * 256])
            for h in range(2):
                c = 2 * c2 + h
                re = first[:R, h * 128 : h * 128 + 128]
                im = first[R:, h * 128 : h * 128 + 128]
                rows = slice(c * R, (c + 1) * R)
                back[rows, 0:128] = (re * ct + im * st).astype(jnp.bfloat16)
                back[rows, 128:256] = (im * ct - re * st).astype(jnp.bfloat16)
        for c in range(few):
            rows = slice(c * R, (c + 1) * R)
            spec[slot, rows, :] = dot(back[rows, :], w2[...])

    def convolve(half_index, slot):
        for u in range(spans):
            flat[u * part : (u + 1) * part, :] = (
                hx[half_index, :, :, u * 128 : (u + 1) * 128].astype(jnp.float32).reshape(part, 128)
            )
        forward(flat, 2)
        ct, st = ct_ref[...], st_ref[...]
        for c in range(few):
            rows = slice(c * R, (c + 1) * R)
            ar, ai = spec[slot, rows, 0:128], spec[slot, rows, 128:256]
            br, bi = spec[2, rows, 0:128], spec[2, rows, 128:256]
            back[rows, 0:128] = (ar * br - ai * bi).astype(jnp.bfloat16)
            back[rows, 128:256] = (ar * bi + ai * br).astype(jnp.bfloat16)
            u = dot(back[rows, :], w2i[...])
            ur_, ui_ = u[:, 0:128], u[:, 128:256]
            bs[0:R, c * 128 : (c + 1) * 128] = (ur_ * ct - ui_ * st).astype(jnp.bfloat16)
            bs[R : 2 * R, c * 128 : (c + 1) * 128] = (ui_ * ct + ur_ * st).astype(jnp.bfloat16)
        scale = 2.0 / (256 * R)
        for c2 in range(few // 2):
            z = dot(f1i[...], bs[:, c2 * 256 : (c2 + 1) * 256]) * scale
            for h in range(2):
                for q in range(per):
                    flat[lines(2 * c2 + h, q), :] = z[q * PEERS : (q + 1) * PEERS, h * 128 : h * 128 + 128]
        gain = low_high(rows_t[9], rows_t[9])[half_index]
        gain = jnp.broadcast_to(gain[None], (PEERS, owned, 128)).reshape(part, 128)
        for u in range(spans):
            rows = slice(u * part, (u + 1) * part)
            skipped = (flat[rows, :] + gain * pf[half_index, rows, :]).astype(jnp.bfloat16).astype(jnp.float32)
            gated = (qf[half_index, rows, :] * skipped).astype(jnp.bfloat16)
            sk[half_index, :, :, u * 128 : (u + 1) * 128] = gated.reshape(PEERS, owned, 128)
        ret[half_index, 0, me] = sk[half_index, me]

    chunks = [(h, u) for h in range(2) for u in range(spans)]

    def emit(c):
        h, u = chunks[c]
        cols = pl.ds(u * 128, 128)
        for plane in range(2):
            each_peer(
                (plane,),
                lambda p, k, dev: send(sk.at[h, p, :, cols], ret.at[h, k, me, :, cols], xsnd.at[k, c], xrcv.at[k, c], dev).start(),
            )

    for i in range(9, 16):
        loads[i].wait()
    forward(pf.at[0], 0)
    all_of(hx.at[0], fs.at[0], fr.at[0]).wait_recv()
    convolve(0, 0)
    emit(0)
    forward(pf.at[1], 1)
    lanes = lax.broadcasted_iota(jnp.int32, (128, 128), 1)
    for b in range(per):
        col = upright(ids_ref[b : b + 1, :])
        for j in range(vocab // 128):
            hot[b * 128 : (b + 1) * 128, j * 128 : (j + 1) * 128] = (col == lanes + 128 * j).astype(jnp.float32).astype(jnp.bfloat16)
    res[...] = dot(hot[...], rt[...])
    emit(1)
    all_of(hx.at[1], fs.at[1], fr.at[1]).wait_recv()
    convolve(1, 1)

    def slot_of(k, yy):
        return (zh if k == 0 else 1 - zh) * 4 + yy

    def piece(c, slot):
        h, u = chunks[c]
        return buf.at[h, slot, u]

    def direct(k, c, upward):
        here = piece(c, slot_of(k, y))
        s, r = (us, ur) if upward else (ds, dr)
        return send(here, here, s.at[k, c], r.at[k, c], {"y": up if upward else down})

    def relay(k, c):
        if k == 1 and c in CROSS:
            here = piece(c, slot_of(0, lax.rem(y + 2, 4)))
            return send(here, here, ls.at[k, c], lr.at[k, c], {"zh": 1 - zh})
        upward = (c + k) % 2 == 0
        here = piece(c, slot_of(k, down if upward else up))
        return send(here, here, ls.at[k, c], lr.at[k, c], {"y": up if upward else down})

    def returned(k, c):
        h, u = chunks[c]
        most = ret.at[h, k, pl.ds(0, PEERS - 1 + k), :, pl.ds(u * 128, 128)]
        return send(most, most, xsnd.at[k, c], xrcv.at[k, c], {"y": up})

    def turn(k, c):
        h, u = chunks[c]
        returned(k, c).wait_recv()
        tiles = ret[h, k, :, :, u * 128 : (u + 1) * 128].astype(jnp.float32).reshape(PEERS // 2, 2, owned, 128)
        for b, rows in enumerate(low_high(tiles[:, 0], tiles[:, 1])):
            buf[h, slot_of(k, y), u, b * 128 : (b + 1) * 128, :] = jnp.transpose(rows.reshape(128, 128)).astype(jnp.bfloat16)
        direct(k, c, True).start()
        direct(k, c, False).start()

    def pass_on(k, c):
        if k == 1 and c in CROSS:
            relay(0, c).wait_recv()
        else:
            direct(k, c, (c + k) % 2 == 0).wait_recv()
        relay(k, c).start()

    def finish(c):
        h, u = chunks[c]
        for k in range(2):
            direct(k, c, (c + k) % 2 == 1).wait_recv()
            if k == 1 and c in CROSS:
                direct(k, c, (c + k) % 2 == 0).wait_recv()
            if not (k == 0 and c in CROSS):
                relay(k, c).wait_recv()
        for b in range(2):
            q = u + b * spans
            rows = slice(q * 128, (q + 1) * 128)
            left = jnp.concatenate([buf[h, j, u, b * 128 : (b + 1) * 128, :] for j in range(TP)], axis=1)
            total = res[rows, :] + dot(left, wo[h].reshape(TP * 128, width))
            if h == 0:
                res[rows, :] = total
            else:
                o_ref[rows, :] = total.astype(jnp.bfloat16)

    emit(2)
    for i in range(16, 20):
        loads[i].wait()
    for s in range(CHUNKS + 3):
        for k in range(2):
            if s < CHUNKS:
                turn(k, s)
            if 0 <= s - 1 < CHUNKS and not (k == 1 and s - 1 in CROSS):
                pass_on(k, s - 1)
        if s + AHEAD < CHUNKS:
            emit(s + AHEAD)
        if s - 2 in CROSS:
            pass_on(1, s - 2)
        if 0 <= s - 3 < CHUNKS:
            finish(s - 3)

    all_of(idall, ids_s, ids_r).wait_send()
    picks_copy.wait_send()
    for h in range(2):
        all_of(hx.at[h], fs.at[h], fr.at[h]).wait_send()
    for c in range(CHUNKS):
        for k in range(2):
            returned(k, c).wait_send()
            direct(k, c, True).wait_send()
            direct(k, c, False).wait_send()
            relay(k, c).wait_send()


def local(token_ids, embed_table, norm_gain, w_in, short_taps, long_filter, skip_gain, w_out):
    vocab, width = embed_table.shape
    T = token_ids.shape[0]
    part = w_in.shape[2]
    owned = part // PEERS
    per = T // 128
    R = PEERS * per
    cols = w_out.shape[1]
    f1, ct, st, w2, w2i, f1i = tables(PEERS, per)
    bf = lambda a: jnp.asarray(a.astype(jnp.bfloat16))
    f32 = lambda a: jnp.asarray(a.astype(np.float32))
    vmem = pl.BlockSpec(memory_space=pltpu.VMEM)
    hbm = pl.BlockSpec(memory_space=pltpu.HBM)
    dma = pltpu.SemaphoreType.DMA
    B, F = jnp.bfloat16, jnp.float32
    V = pltpu.VMEM
    operands = (
        token_ids.reshape(per, 128),
        norm_gain.reshape(1, width),
        short_taps,
        skip_gain.reshape(part // 128, 128),
        f32(ct),
        f32(st),
        embed_table,
        jnp.transpose(w_in, (1, 0, 2)),
        long_filter.reshape(PEERS, owned, T),
        w_out.reshape(TP, 2, 2, part // 4, cols),
        bf(f1),
        bf(w2),
        bf(w2i),
        bf(f1i),
    )
    return pl.pallas_call(
        block_kernel,
        out_shape=jax.ShapeDtypeStruct((T, cols), B),
        in_specs=[hbm] * 14,
        out_specs=vmem,
        scratch_shapes=[
            V((per, 128), jnp.int32),
            V((1, width), F),
            V(short_taps.shape, F),
            V((part // 128, 128), F),
            V(ct.shape, F),
            V(st.shape, F),
            V((PEERS, owned, T), B),
            V((2, PEERS, owned, T // 2), B),
            V((vocab // 2, width), B),
            V((vocab // 2, width), B),
            V((width, 384), B),
            V((vocab, cols), B),
            V((2, vocab // 256, 4 * owned, 128), B),
            V((vocab // 128, 4 * owned, 128), B),
            V((T, vocab), B),
            V((2, TP, part // 2, cols), B),
            V(f1.shape, B),
            V(w2.shape, B),
            V(w2i.shape, B),
            V(f1i.shape, B),
            V((per // 2, 128), jnp.int32),
            V((PEERS, per // 2, 128), jnp.int32),
            V((128, 128), F),
            V((10, owned, 128), F),
            V((2, PEERS, owned, T // 2), B),
            V((2, per // 2 * part, 128), F),
            V((2, per // 2 * part, 128), F),
            V((T, cols), F),
            V((per // 2 * part, 128), F),
            V((R, owned // 2 * 128), B),
            V((3, owned // 2 * R, 256), F),
            V((owned // 2 * R, 256), B),
            V((2 * R, owned // 2 * 128), B),
            V((2, PEERS, owned, T // 2), B),
            V((2, 2, PEERS, owned, T // 2), B),
            V((2, TP, per // 2, 256, part // 2), B),
            dma((20,)),
            dma,
            dma,
            dma((2,)),
            dma((2,)),
            dma,
            dma,
        ]
        + [dma((2, CHUNKS))] * 8,
        compiler_params=pltpu.CompilerParams(collective_id=0, has_side_effects=True, vmem_limit_bytes=48 * 2**20),
        name="block",
    )(*(pltpu.with_memory_space_constraint(a, pltpu.HBM) for a in operands))


def solution(mesh):
    finer = Mesh(mesh.devices.reshape(4, 4, 2, 2, 4), ("x", "zl", "core", "zh", "y"))
    tp = ("zh", "y")
    in_specs = (
        P(CTX),
        P(),
        P(),
        P(None, None, tp),
        P(None, None, tp),
        P(tp, CTX),
        P(tp),
        P(None, tp),
    )
    return jax.shard_map(local, mesh=finer, in_specs=in_specs, out_specs=P(CTX, tp), check_vma=False)
```

```python
import functools
import math

import jax
import jax.numpy as jnp
import numpy as np
from jax import lax
from jax.experimental import pallas as pl
from jax.experimental.pallas import tpu as pltpu
from jax.sharding import Mesh
from jax.sharding import PartitionSpec as P

CTX = ("x", "zl", "core")
MESH = pl.DeviceIdType.MESH
PEERS = 32
TP = 8
norm_eps = 1e-06


@functools.lru_cache(maxsize=None)
def tables(peers, per):
    R = peers * per
    N = 256 * R
    order = (np.arange(per)[:, None] + per * np.arange(peers)[None, :]).reshape(-1)
    k1 = np.arange(R) + 0.5
    a1 = 2 * np.pi * np.outer(k1, order) / (2 * R)
    f1 = np.concatenate([np.cos(a1), -np.sin(a1)], 0)
    at = 2 * np.pi * np.outer(k1, np.arange(128)) / N
    a2 = 2 * np.pi * (np.outer(np.arange(128), np.arange(128)) % 128) / 128
    c, s = np.cos(a2), np.sin(a2)
    w2 = np.block([[c, -s], [s, c]])
    w2i = np.block([[c, s], [-s, c]])
    f1i = np.concatenate([np.cos(a1.T), -np.sin(a1.T)], 1)
    return f1, np.cos(at), np.sin(at), w2, w2i, f1i


def peer_of(p):
    return {"x": p // 8, "zl": lax.rem(p // 2, 4), "core": lax.rem(p, 2)}


def ctx_index():
    return lax.axis_index("x") * 8 + lax.axis_index("zl") * 2 + lax.axis_index("core")


def dot(a, b):
    return jnp.dot(a, b, preferred_element_type=jnp.float32)


def send(src, dst, s, r, dev):
    return pltpu.make_async_remote_copy(
        src_ref=src, dst_ref=dst, send_sem=s, recv_sem=r, device_id=dev, device_id_type=MESH
    )


CHUNKS = 6
AHEAD = 3
CROSS = (1, 2)
UNROLL = 3


def normalize(tv, gain_ref, nv, first, last):
    width = tv.shape[1]

    @pl.loop(first, last, unroll=2)
    def _(r):
        rows = pl.ds(pl.multiple_of(r * 32, 32), 32)
        acc = jnp.zeros((32, 128), jnp.float32)
        for j in range(width // 128):
            x = tv[rows, j * 128 : (j + 1) * 128].astype(jnp.float32)
            acc += x * x
        scale = lax.rsqrt(jnp.sum(acc, axis=1, keepdims=True) * (1.0 / width) + norm_eps)
        for j in range(width // 128):
            cols = slice(j * 128, (j + 1) * 128)
            x = tv[rows, cols].astype(jnp.float32)
            nv[rows, cols] = (x * scale * gain_ref[:, cols]).astype(jnp.bfloat16)


def upright(row):
    return jnp.transpose(jnp.broadcast_to(row, (128, 128)))


def low_high(a, b):
    axis = a.ndim - 2
    first = lax.broadcasted_iota(jnp.int32, a.shape, axis) < 4
    return jnp.where(first, a, pltpu.roll(b, 4, axis)), jnp.where(first, pltpu.roll(a, 4, axis), b)


def block_kernel(
    ids_hbm, gain_hbm, taps_hbm, skip_hbm, ct_hbm, st_hbm, table_hbm, w3_hbm, filt_hbm, wo_hbm, f1_hbm, w2_hbm, w2i_hbm, f1i_hbm,
    o_ref,
    ids_ref, gain_ref, taps_ref, skip_ref, ct_ref, st_ref, fv, fsend, tv, nv, wv, rt, halves, picks, hot, wo, f1, w2, w2i, f1i,
    idpair, idall, column, rows_t, hx, pf, qf, res, flat, xs, spec, back, bs, sk, ret, buf,
    ld, ids_s, ids_r, fs, fr, pk_s, pk_r, xsnd, xrcv, us, ur, ds, dr, ls, lr,
):
    x, zl, core = lax.axis_index("x"), lax.axis_index("zl"), lax.axis_index("core")
    me = ctx_index()
    zh, y = lax.axis_index("zh"), lax.axis_index("y")
    own = zh * 4 + y
    up, down = lax.rem(y + 1, 4), lax.rem(y + 3, 4)
    mine = tv.shape[0]
    vocab = 2 * mine
    owned = fv.shape[1]
    few = owned // 2
    part = PEERS * owned
    T = res.shape[0]
    width = o_ref.shape[1]
    per = T // 128
    spans = per // 2
    R = PEERS * per
    half = me // 16
    pair = pl.multiple_of(lax.rem(me, 16) // 2 * owned, owned)

    def owned_rows(ref, base):
        return low_high(
            ref[pl.ds(pl.multiple_of(base + pair, owned), owned), :], ref[pl.ds(pl.multiple_of(base + 64 + pair, owned), owned), :]
        )

    def each_peer(planes, fn):
        planes = range(planes) if isinstance(planes, int) else planes

        def chip(t, skip_self):
            px, pz = lax.rem(x + t // 4, 4), lax.rem(zl + lax.rem(t, 4), 4)
            for dc in range(2):
                pc = lax.rem(core + dc, 2)
                p = px * 8 + pz * 2 + pc
                for k in planes:
                    if not (skip_self and dc == 0 and k == 0):
                        dev = {"x": px, "zl": pz, "core": pc}
                        if k == 1:
                            dev["zh"] = 1 - zh
                        fn(p, k, dev)

        def go(t, carry):
            chip(t, False)
            return carry

        lax.fori_loop(1, 16, go, 0, unroll=UNROLL)
        chip(0, True)

    bar = pltpu.get_barrier_semaphore()

    def greet(dev):
        pl.semaphore_signal(bar, inc=1, device_id=dev, device_id_type=MESH)

    each_peer(2, lambda p, k, dev: greet(dev))
    greet({"y": up})
    greet({"y": down})

    pairs = (
        [
            (ids_hbm, ids_ref),
            (filt_hbm, fv),
            (table_hbm.at[pl.ds(pl.multiple_of(core * mine, mine), mine)], tv),
            (gain_hbm, gain_ref),
            (taps_hbm, taps_ref),
            (skip_hbm, skip_ref),
        ]
        + [(w3_hbm.at[s, :, pl.ds(pl.multiple_of(half * 128, 128), 128)], wv.at[:, pl.ds(s * 128, 128)]) for s in range(3)]
        + [
            (ct_hbm, ct_ref),
            (st_hbm, st_ref),
            (f1_hbm, f1),
            (w2_hbm, w2),
            (w2i_hbm, w2i),
            (f1i_hbm, f1i),
            (table_hbm.at[:, pl.ds(pl.multiple_of(own * width, width), width)], rt),
        ]
        + [(wo_hbm.at[:, a, h], wo.at[h, :, pl.ds(64 * a, 64)]) for a in range(2) for h in range(2)]
    )
    loads = [pltpu.make_async_copy(a, b, ld.at[i]) for i, (a, b) in enumerate(pairs)]
    for c in loads:
        c.start()
    for i in range(2):
        loads[i].wait()
    idpair[...] = ids_ref[0:spans, :] + ids_ref[spans:per, :] * 65536
    for h in range(2):
        for a in range(2):
            t0 = a * 16 + h * 8
            tiles = fv[t0 : t0 + 8].astype(jnp.float32)
            even, odd = low_high(tiles[:, :, : T // 2], tiles[:, :, T // 2 :])
            fsend[h, a * 16 : (a + 1) * 16] = jnp.stack([even, odd], axis=1).reshape(16, owned, T // 2).astype(jnp.bfloat16)
    pl.semaphore_wait(bar, 2 * PEERS + 1)

    each_peer(1, lambda p, k, dev: send(idpair, idall.at[me], ids_s, ids_r, dev).start())

    def send_filter(h):
        each_peer(1, lambda p, k, dev: send(fsend.at[h, p], hx.at[h, me], fs.at[h], fr.at[h], dev).start())

    send_filter(0)

    def all_of(ref, s, r):
        most = ref.at[pl.ds(0, PEERS - 1)]
        return send(most, most, s, r, {"y": up})

    idall[me] = idpair[...]
    for h in range(2):
        hx[h, me] = fsend[h, me]

    for i in range(2, 4):
        loads[i].wait()
    normalize(tv, gain_ref, nv, 0, mine // 32)
    for s in range(3):
        loads[6 + s].wait()
    for n0, n1 in ((0, 256), (256, 384)):
        projected = dot(nv[...], wv[:, n0:n1]).astype(jnp.bfloat16).astype(jnp.float32)
        for n in range(n0, n1, 128):
            for v in range(mine // 128):
                row = (n // 128 * 2 + v) * 128
                flat[row : row + 128, :] = jnp.transpose(projected[v * 128 : (v + 1) * 128, n - n0 : n - n0 + 128])
    for v in range(mine // 128):
        found = [owned_rows(flat, (s * 2 + v) * 128) for s in range(3)]
        for c in range(2):
            rows = [f[c] for f in found] + [jnp.zeros((owned, 128), jnp.float32)]
            halves[c, v] = jnp.concatenate(rows, axis=0).astype(jnp.bfloat16)
    groups = vocab // 128
    picks_copy = send(halves.at[1 - core], picks.at[pl.ds(2 * core, 2)], pk_s, pk_r, {"core": 1 - core})
    picks_copy.start()
    picks[pl.ds(2 * core, 2)] = halves[core]

    for i in range(4, 6):
        loads[i].wait()

    def own_column(row_a, row_b, to):
        column[...] = upright(jnp.where(half == 0, row_a, row_b))
        low, high = owned_rows(column, 0)
        rows_t[to] = jnp.where(core == 0, low, high)

    for r in range(3):
        for s in range(3):
            own_column(taps_ref[r, s : s + 1, 0:128], taps_ref[r, s : s + 1, 128:256], r * 3 + s)
    own_column(skip_ref[0:1, :], skip_ref[1:2, :], 9)

    all_of(idall, ids_s, ids_r).wait_recv()
    send_filter(1)
    picks_copy.wait_recv()
    table_rows = picks[...].astype(jnp.float32)[:, : 3 * owned, :].reshape(groups * 3 * owned, 128).astype(jnp.bfloat16)
    lane = lax.broadcasted_iota(jnp.int32, (owned, 128), 1)
    token = lax.broadcasted_iota(jnp.int32, (128, 128), 0)

    def positions(i, carry):
        products, queries = [], []
        for q2 in range(per // 2):
            both = [idall[i, q % spans : q % spans + 1, :] for q in (2 * q2, 2 * q2 + 1)]
            both = [ids & 65535 if 2 * q2 + h < spans else ids >> 16 for h, ids in enumerate(both)]
            hits = [(jnp.broadcast_to(ids & 127, (128, 128)) == token).astype(jnp.float32).astype(jnp.bfloat16) for ids in both]
            chosen = dot(table_rows, jnp.concatenate(hits, axis=1))
            for h in range(2):
                group = jnp.broadcast_to(both[h] >> 7, (owned, 128))
                short, later = [], []
                for s in range(3):
                    of = [
                        chosen[(v * 3 + s) * owned : (v * 3 + s + 1) * owned, h * 128 : (h + 1) * 128] for v in range(groups)
                    ]
                    now = of[0]
                    for v in range(1, groups):
                        now = jnp.where(group == v, of[v], now)
                    by1, by2 = pltpu.roll(now, 1, 1), pltpu.roll(now, 2, 1)
                    before1, before2 = carry[s]
                    one = jnp.where(lane < 1, before1, by1)
                    two = jnp.where(lane < 2, before2, by2)
                    short.append(
                        (rows_t[s] * now + rows_t[3 + s] * one + rows_t[6 + s] * two).astype(jnp.bfloat16).astype(jnp.float32)
                    )
                    later.append((by1, by2))
                carry = tuple(later)
                products.append((short[1] * short[2]).astype(jnp.bfloat16).astype(jnp.float32))
                queries.append(short[0])
        for u in range(spans):
            rows = pl.ds(pl.multiple_of(u * part + i * owned, owned), owned)
            pf[0, rows, :], pf[1, rows, :] = low_high(products[u], products[u + spans])
            qf[0, rows, :], qf[1, rows, :] = low_high(queries[u], queries[u + spans])
        return carry

    nothing = jnp.zeros((owned, 128), jnp.float32)
    lax.fori_loop(0, PEERS, positions, ((nothing, nothing),) * 3, unroll=8)

    def lines(c, q):
        return pl.ds(q % spans * part + c + few * (q // spans), PEERS, stride=owned)

    def forward(src, slot):
        for c in range(few):
            for q in range(per):
                xs[q * PEERS : (q + 1) * PEERS, c * 128 : (c + 1) * 128] = src[lines(c, q), :].astype(jnp.bfloat16)
        ct, st = ct_ref[...], st_ref[...]
        for c2 in range(few // 2):
            first = dot(f1[...], xs[:, c2 * 256 : (c2 + 1) * 256])
            for h in range(2):
                c = 2 * c2 + h
                re = first[:R, h * 128 : h * 128 + 128]
                im = first[R:, h * 128 : h * 128 + 128]
                rows = slice(c * R, (c + 1) * R)
                back[rows, 0:128] = (re * ct + im * st).astype(jnp.bfloat16)
                back[rows, 128:256] = (im * ct - re * st).astype(jnp.bfloat16)
        for c in range(few):
            rows = slice(c * R, (c + 1) * R)
            spec[slot, rows, :] = dot(back[rows, :], w2[...])

    def convolve(half_index, slot):
        for u in range(spans):
            flat[u * part : (u + 1) * part, :] = (
                hx[half_index, :, :, u * 128 : (u + 1) * 128].astype(jnp.float32).reshape(part, 128)
            )
        forward(flat, 2)
        ct, st = ct_ref[...], st_ref[...]
        for c in range(few):
            rows = slice(c * R, (c + 1) * R)
            ar, ai = spec[slot, rows, 0:128], spec[slot, rows, 128:256]
            br, bi = spec[2, rows, 0:128], spec[2, rows, 128:256]
            back[rows, 0:128] = (ar * br - ai * bi).astype(jnp.bfloat16)
            back[rows, 128:256] = (ar * bi + ai * br).astype(jnp.bfloat16)
            u = dot(back[rows, :], w2i[...])
            ur_, ui_ = u[:, 0:128], u[:, 128:256]
            bs[0:R, c * 128 : (c + 1) * 128] = (ur_ * ct - ui_ * st).astype(jnp.bfloat16)
            bs[R : 2 * R, c * 128 : (c + 1) * 128] = (ui_ * ct + ur_ * st).astype(jnp.bfloat16)
        scale = 2.0 / (256 * R)
        for c2 in range(few // 2):
            z = dot(f1i[...], bs[:, c2 * 256 : (c2 + 1) * 256]) * scale
            for h in range(2):
                for q in range(per):
                    flat[lines(2 * c2 + h, q), :] = z[q * PEERS : (q + 1) * PEERS, h * 128 : h * 128 + 128]
        gain = low_high(rows_t[9], rows_t[9])[half_index]
        gain = jnp.broadcast_to(gain[None], (PEERS, owned, 128)).reshape(part, 128)
        for u in range(spans):
            rows = slice(u * part, (u + 1) * part)
            skipped = (flat[rows, :] + gain * pf[half_index, rows, :]).astype(jnp.bfloat16).astype(jnp.float32)
            gated = (qf[half_index, rows, :] * skipped).astype(jnp.bfloat16)
            sk[half_index, :, :, u * 128 : (u + 1) * 128] = gated.reshape(PEERS, owned, 128)
        ret[half_index, 0, me] = sk[half_index, me]

    chunks = [(h, u) for h in range(2) for u in range(spans)]

    def emit(c):
        h, u = chunks[c]
        cols = pl.ds(u * 128, 128)
        for plane in range(2):
            each_peer(
                (plane,),
                lambda p, k, dev: send(sk.at[h, p, :, cols], ret.at[h, k, me, :, cols], xsnd.at[k, c], xrcv.at[k, c], dev).start(),
            )

    for i in range(9, 16):
        loads[i].wait()
    forward(pf.at[0], 0)
    all_of(hx.at[0], fs.at[0], fr.at[0]).wait_recv()
    convolve(0, 0)
    emit(0)
    forward(pf.at[1], 1)
    lanes = lax.broadcasted_iota(jnp.int32, (128, 128), 1)
    for b in range(per):
        col = upright(ids_ref[b : b + 1, :])
        for j in range(vocab // 128):
            hot[b * 128 : (b + 1) * 128, j * 128 : (j + 1) * 128] = (col == lanes + 128 * j).astype(jnp.float32).astype(jnp.bfloat16)
    res[...] = dot(hot[...], rt[...])
    emit(1)
    all_of(hx.at[1], fs.at[1], fr.at[1]).wait_recv()
    convolve(1, 1)

    def slot_of(k, yy):
        return (zh if k == 0 else 1 - zh) * 4 + yy

    def piece(c, slot):
        h, u = chunks[c]
        return buf.at[h, slot, u]

    def direct(k, c, upward):
        here = piece(c, slot_of(k, y))
        s, r = (us, ur) if upward else (ds, dr)
        return send(here, here, s.at[k, c], r.at[k, c], {"y": up if upward else down})

    def relay(k, c):
        if k == 1 and c in CROSS:
            here = piece(c, slot_of(0, lax.rem(y + 2, 4)))
            return send(here, here, ls.at[k, c], lr.at[k, c], {"zh": 1 - zh})
        upward = (c + k) % 2 == 0
        here = piece(c, slot_of(k, down if upward else up))
        return send(here, here, ls.at[k, c], lr.at[k, c], {"y": up if upward else down})

    def returned(k, c):
        h, u = chunks[c]
        most = ret.at[h, k, pl.ds(0, PEERS - 1 + k), :, pl.ds(u * 128, 128)]
        return send(most, most, xsnd.at[k, c], xrcv.at[k, c], {"y": up})

    def turn(k, c):
        h, u = chunks[c]
        returned(k, c).wait_recv()
        tiles = ret[h, k, :, :, u * 128 : (u + 1) * 128].astype(jnp.float32).reshape(PEERS // 2, 2, owned, 128)
        for b, rows in enumerate(low_high(tiles[:, 0], tiles[:, 1])):
            buf[h, slot_of(k, y), u, b * 128 : (b + 1) * 128, :] = jnp.transpose(rows.reshape(128, 128)).astype(jnp.bfloat16)
        direct(k, c, True).start()
        direct(k, c, False).start()

    def pass_on(k, c):
        if k == 1 and c in CROSS:
            relay(0, c).wait_recv()
        else:
            direct(k, c, (c + k) % 2 == 0).wait_recv()
        relay(k, c).start()

    def finish(c):
        h, u = chunks[c]
        for k in range(2):
            direct(k, c, (c + k) % 2 == 1).wait_recv()
            if k == 1 and c in CROSS:
                direct(k, c, (c + k) % 2 == 0).wait_recv()
            if not (k == 0 and c in CROSS):
                relay(k, c).wait_recv()
        for b in range(2):
            q = u + b * spans
            rows = slice(q * 128, (q + 1) * 128)
            left = jnp.concatenate([buf[h, j, u, b * 128 : (b + 1) * 128, :] for j in range(TP)], axis=1)
            total = res[rows, :] + dot(left, wo[h].reshape(TP * 128, width))
            if h == 0:
                res[rows, :] = total
            else:
                o_ref[rows, :] = total.astype(jnp.bfloat16)

    emit(2)
    for i in range(16, 20):
        loads[i].wait()
    for s in range(CHUNKS + 3):
        for k in range(2):
            if s < CHUNKS:
                turn(k, s)
            if 0 <= s - 1 < CHUNKS and not (k == 1 and s - 1 in CROSS):
                pass_on(k, s - 1)
        if s + AHEAD < CHUNKS:
            emit(s + AHEAD)
        if s - 2 in CROSS:
            pass_on(1, s - 2)
        if 0 <= s - 3 < CHUNKS:
            finish(s - 3)

    all_of(idall, ids_s, ids_r).wait_send()
    picks_copy.wait_send()
    for h in range(2):
        all_of(hx.at[h], fs.at[h], fr.at[h]).wait_send()
    for c in range(CHUNKS):
        for k in range(2):
            returned(k, c).wait_send()
            direct(k, c, True).wait_send()
            direct(k, c, False).wait_send()
            relay(k, c).wait_send()


def local(token_ids, embed_table, norm_gain, w_in, short_taps, long_filter, skip_gain, w_out):
    vocab, width = embed_table.shape
    T = token_ids.shape[0]
    part = w_in.shape[2]
    owned = part // PEERS
    per = T // 128
    R = PEERS * per
    cols = w_out.shape[1]
    f1, ct, st, w2, w2i, f1i = tables(PEERS, per)
    bf = lambda a: jnp.asarray(a.astype(jnp.bfloat16))
    f32 = lambda a: jnp.asarray(a.astype(np.float32))
    vmem = pl.BlockSpec(memory_space=pltpu.VMEM)
    hbm = pl.BlockSpec(memory_space=pltpu.HBM)
    dma = pltpu.SemaphoreType.DMA
    B, F = jnp.bfloat16, jnp.float32
    V = pltpu.VMEM
    operands = (
        token_ids.reshape(per, 128),
        norm_gain.reshape(1, width),
        short_taps,
        skip_gain.reshape(part // 128, 128),
        f32(ct),
        f32(st),
        embed_table,
        jnp.transpose(w_in, (1, 0, 2)),
        long_filter.reshape(PEERS, owned, T),
        w_out.reshape(TP, 2, 2, part // 4, cols),
        bf(f1),
        bf(w2),
        bf(w2i),
        bf(f1i),
    )
    return pl.pallas_call(
        block_kernel,
        out_shape=jax.ShapeDtypeStruct((T, cols), B),
        in_specs=[hbm] * 14,
        out_specs=vmem,
        scratch_shapes=[
            V((per, 128), jnp.int32),
            V((1, width), F),
            V(short_taps.shape, F),
            V((part // 128, 128), F),
            V(ct.shape, F),
            V(st.shape, F),
            V((PEERS, owned, T), B),
            V((2, PEERS, owned, T // 2), B),
            V((vocab // 2, width), B),
            V((vocab // 2, width), B),
            V((width, 384), B),
            V((vocab, cols), B),
            V((2, vocab // 256, 4 * owned, 128), B),
            V((vocab // 128, 4 * owned, 128), B),
            V((T, vocab), B),
            V((2, TP, part // 2, cols), B),
            V(f1.shape, B),
            V(w2.shape, B),
            V(w2i.shape, B),
            V(f1i.shape, B),
            V((per // 2, 128), jnp.int32),
            V((PEERS, per // 2, 128), jnp.int32),
            V((128, 128), F),
            V((10, owned, 128), F),
            V((2, PEERS, owned, T // 2), B),
            V((2, per // 2 * part, 128), F),
            V((2, per // 2 * part, 128), F),
            V((T, cols), F),
            V((per // 2 * part, 128), F),
            V((R, owned // 2 * 128), B),
            V((3, owned // 2 * R, 256), F),
            V((owned // 2 * R, 256), B),
            V((2 * R, owned // 2 * 128), B),
            V((2, PEERS, owned, T // 2), B),
            V((2, 2, PEERS, owned, T // 2), B),
            V((2, TP, per // 2, 256, part // 2), B),
            dma((20,)),
            dma,
            dma,
            dma((2,)),
            dma((2,)),
            dma,
            dma,
        ]
        + [dma((2, CHUNKS))] * 8,
        compiler_params=pltpu.CompilerParams(collective_id=0, has_side_effects=True, vmem_limit_bytes=48 * 2**20),
        name="block",
    )(*(pltpu.with_memory_space_constraint(a, pltpu.HBM) for a in operands))


def solution(mesh):
    finer = Mesh(mesh.devices.reshape(4, 4, 2, 2, 4), ("x", "zl", "core", "zh", "y"))
    tp = ("zh", "y")
    in_specs = (
        P(CTX),
        P(),
        P(),
        P(None, None, tp),
        P(None, None, tp),
        P(tp, CTX),
        P(tp),
        P(None, tp),
    )
    return jax.shard_map(local, mesh=finer, in_specs=in_specs, out_specs=P(CTX, tp), check_vma=False)
```
